256 devices in a mesh: node: 64 (over z, x, core), rep: 4 (over y).
Axes of the slice: x: 4, y: 4, z: 8, core: 2. Of those that a mesh axis runs over, the one named last changes fastest.
Arguments:
- features: bfloat16 [1310720, 256], P('node'), may hold values from -6 to 6
- w_in: bfloat16 [256, 256], replicated, may hold values from -0.375 to 0.375
- w_out: bfloat16 [256, 256], replicated, may hold values from -0.375 to 0.375
- pos_src: int32 [64, 4, 64, 2], P('node', 'rep'), may hold values from 0 to 159
- pos_dst: int32 [64, 4, 64, 2], P('node', 'rep'), may hold values from 0 to 159
- counts: int32 [64, 4, 64], P('node', 'rep'), may hold values from 1 to 2, as said below
- neg_blocks: int32 [64, 2], P('node'), may hold values from 0 to 159
- neg_pick: int32 [64, 4, 64, 2], P('node', 'rep'), may hold values from 0 to 127
Outputs:
- pos_scores: float32 [64, 4, 64, 2, 128], P('node', 'rep')
- neg_term: float32 [64, 4, 64, 2, 128], P('node', 'rep')
- loss: float32 [], replicated
The draws below stay inside these ranges and needn't reach their ends.
Inputs may be any that keep to these rules, and one draw needn't show every extreme that they name: `counts`: each entry is at most 2; in every draw one owner receives 2 live slots from every device.
All inputs are finite; a program needn't handle non-finite values.
Results may differ from the reference program's by a relative error of at most 0.0027.
Values may be sent and summed in bfloat16 or wider, within the bound.
A program may use at most 192 MiB of HBM per device.

```python
import jax
import jax.numpy as jnp
from jax import lax

D = 256
HID = 256
BLK = 128
BLOCKS_DEV = 160
CAP = 2
NEG = 2
NODES = 1310720
POOL = 128
N_NODE = 64
N_REP = 4


def draw_counts(key, part):
    first = jax.random.fold_in(key, 11)
    second = jax.random.fold_in(key, 12)
    third = jax.random.fold_in(key, 13)
    heat = jax.random.randint(first, (N_NODE,), 0, 3)
    uneven = jax.random.randint(second, (N_NODE, N_REP, N_NODE), 0, 4)
    level = jnp.minimum(CAP, (uneven + heat[None, None, :] + 2) // 2)
    hottest = jax.random.randint(third, (), 0, N_NODE)
    owners = jnp.arange(N_NODE)[None, None, :]
    return jnp.where(owners == hottest, CAP, level).astype(jnp.int32)


def place_ends(entries, own_key, least, largest):
    shape = entries.shape
    place = [jax.random.randint(jax.random.fold_in(own_key, axis), (), 0, shape[axis]) for axis in range(len(shape))]
    entries = entries.at[tuple(place)].set(least)
    longest = shape.index(max(shape))
    place[longest] = (place[longest] + 1) % shape[longest]
    return entries.at[tuple(place)].set(largest)


def shard_levels(stream_key, dims, cuts, low, largest):
    level, own = 1.0, jax.random.fold_in(stream_key, 6)
    for dim, shards_of in cuts:
        heights = jnp.exp(jax.random.uniform(jax.random.fold_in(own, dim), (shards_of,), jnp.float32, low / len(cuts), largest / len(cuts)))
        level = level * jnp.repeat(heights, dims[dim] // shards_of).reshape([-1 if axis == dim else 1 for axis in range(len(dims))])
    return level


def centred(stream_key, shape, spread, limit, split=(), held_as=jnp.bfloat16):
    result = jax.random.normal(stream_key, shape, jnp.float32) * spread
    if len(split) > 0:
        result = shard_levels(stream_key, shape, split, -0.22, 0.18) * result
    return jnp.clip(result, min=-limit, max=limit).astype(held_as)


def setup_inputs(seed: int = 0) -> dict:
    streams_of = jax.random.split(jax.random.key(seed), 9)
    features = centred(streams_of[0], (NODES, D), 1.0, 6.0, ((0, 64),))
    w_in = centred(streams_of[1], (D, HID), D ** -0.5, 0.375)
    w_out = centred(streams_of[2], (HID, D), HID ** -0.5, 0.375)
    pos_src = place_ends(jax.random.randint(streams_of[3], (N_NODE, N_REP, N_NODE, CAP), 0, BLOCKS_DEV), jax.random.fold_in(streams_of[3], 1), 0, BLOCKS_DEV - 1).astype(jnp.int32)
    pos_dst = place_ends(jax.random.randint(streams_of[4], (N_NODE, N_REP, N_NODE, CAP), 0, BLOCKS_DEV), jax.random.fold_in(streams_of[4], 1), 0, BLOCKS_DEV - 1).astype(jnp.int32)
    counts = draw_counts(jax.random.fold_in(streams_of[8], 71), 0)
    neg_blocks = place_ends(jax.random.randint(streams_of[6], (N_NODE, NEG), 0, BLOCKS_DEV), jax.random.fold_in(streams_of[6], 1), 0, BLOCKS_DEV - 1).astype(jnp.int32)
    neg_pick = place_ends(jax.random.randint(streams_of[7], (N_NODE, N_REP, N_NODE, CAP), 0, POOL), jax.random.fold_in(streams_of[7], 1), 0, POOL - 1).astype(jnp.int32)
    return dict(features=features, w_in=w_in, w_out=w_out, pos_src=pos_src, pos_dst=pos_dst, counts=counts, neg_blocks=neg_blocks, neg_pick=neg_pick)


def reference(features, w_in, w_out, pos_src, pos_dst, counts, neg_blocks, neg_pick):
    hidden = jax.nn.silu(jnp.dot(features, w_in, preferred_element_type=jnp.float32)).astype(jnp.bfloat16)
    embed = jnp.dot(hidden, w_out, preferred_element_type=jnp.float32).astype(jnp.bfloat16)
    width = embed.shape[1]
    allblk = embed.reshape(N_NODE, BLOCKS_DEV, BLK, width)
    owner_ids = jnp.arange(N_NODE, dtype=jnp.int32)
    pool = allblk[owner_ids[:, None], neg_blocks].reshape(N_NODE * NEG, BLK, width)
    scale = 1.0 / (width ** 0.5)

    def per_node(index):
        mine = allblk[index]
        source = mine[pos_src[index]].astype(jnp.float32)
        target = allblk[owner_ids[None, :, None], pos_dst[index]].astype(jnp.float32)
        cand = pool[neg_pick[index]].astype(jnp.float32)
        raw_pos = jnp.einsum('rocbd,rocbd->rocb', source, target) * scale
        scores = jnp.einsum('rocbd,rocsd->rocbs', source, cand) * scale
        live = jnp.arange(CAP, dtype=jnp.int32)[None, None, :] < counts[index][:, :, None]
        livex = live[..., None]
        pos_out = jnp.where(livex, raw_pos, 0.0)
        neg_out = jnp.where(livex, jnp.mean(jax.nn.softplus(scores), axis=-1), 0.0)
        pos_loss = jnp.sum(jnp.where(livex, jax.nn.softplus(-raw_pos), 0.0))
        return pos_out, neg_out, pos_loss, jnp.sum(neg_out)

    pos_scores, neg_term, pos_losses, neg_sums = lax.map(per_node, jnp.arange(N_NODE, dtype=jnp.int32))
    total = jnp.sum(counts).astype(jnp.float32)
    loss = (jnp.sum(pos_losses) + jnp.sum(neg_sums)) / (BLK * total)
    return pos_scores, neg_term, loss
```

```python
import functools

import jax
import jax.numpy as jnp
from jax import lax
from jax.experimental import pallas as pl
from jax.experimental.pallas import tpu as pltpu
from jax.sharding import PartitionSpec as P

BLK = 128
ALL = ("node", "rep")
VMEM = pl.BlockSpec(memory_space=pltpu.VMEM)
SMEM = pl.BlockSpec(memory_space=pltpu.SMEM)


def silu(v):
    return v / (1.0 + jnp.exp(-v))


def encode(rows_in, w_in, w_out):
    hidden = jax.nn.silu(jnp.dot(rows_in, w_in, preferred_element_type=jnp.float32)).astype(
        jnp.bfloat16
    )
    return jnp.dot(hidden, w_out, preferred_element_type=jnp.float32).astype(jnp.bfloat16)


def rows_kernel(part_ref, x_ref, w_in_ref, w_out_ref, out_ref):
    group, rows, width = x_ref.shape
    x = x_ref[...].reshape(group * rows, width)
    h = jnp.dot(x, w_in_ref[...], preferred_element_type=jnp.float32)
    h = silu(h).astype(jnp.bfloat16)
    e = jnp.dot(h, w_out_ref[...], preferred_element_type=jnp.float32).astype(jnp.bfloat16)
    n = group * rows
    i = lax.broadcasted_iota(jnp.int32, (n, n), 0)
    j = lax.broadcasted_iota(jnp.int32, (n, n), 1)
    perm = jnp.where(j == (i % group) * rows + i // group, 1.0, 0.0).astype(jnp.bfloat16)
    t = jnp.dot(perm, e, preferred_element_type=jnp.float32).astype(jnp.bfloat16)
    half = width // 2
    out_ref[:, 0] = t[:, :half].reshape(rows, group, half)
    out_ref[:, 1] = t[:, half:].reshape(rows, group, half)


def rows_of_blocks(features, w_in, w_out, parts, group=16):
    total, width = features.shape
    blocks = total // BLK
    rows = BLK // parts
    part = lax.axis_index("rep").astype(jnp.int32).reshape(1)
    return pl.pallas_call(
        rows_kernel,
        grid_spec=pltpu.PrefetchScalarGridSpec(
            num_scalar_prefetch=1,
            grid=(blocks // group,),
            in_specs=[
                pl.BlockSpec((group, rows, width), lambda g, p: (g, p[0], 0)),
                pl.BlockSpec((width, width), lambda g, p: (0, 0)),
                pl.BlockSpec((width, width), lambda g, p: (0, 0)),
            ],
            out_specs=pl.BlockSpec((rows, 2, group, width // 2), lambda g, p: (0, 0, g, 0)),
        ),
        out_shape=jax.ShapeDtypeStruct((rows, 2, blocks, width // 2), jnp.bfloat16),
        cost_estimate=pl.CostEstimate(
            flops=2 * blocks * rows * width * (2 * width + group * rows),
            bytes_accessed=4 * blocks * rows * width,
            transcendentals=blocks * rows * width,
        ),
        name="rows",
    )(part, features.reshape(blocks, BLK, width), w_in, w_out)


def hub_kernel(scale, rows_ref, src_ref, dst_ref, out_ref, ends_ref):
    nodes, blocks, width = rows_ref.shape
    edges = src_ref.shape[1]
    lane = lax.broadcasted_iota(jnp.int32, (edges, blocks), 1)
    per = edges // nodes

    def pick(ids, node):
        hot = jnp.where(ids == lane, 1.0, 0.0).astype(jnp.bfloat16)
        return jnp.dot(hot, rows_ref[node], preferred_element_type=jnp.float32)

    def ends(g, _):
        for k in range(8):
            node = g * 8 + k
            got = pick(dst_ref[g, :, k : k + 1], node)
            ends_ref[node] = got.reshape(nodes, per, width)
        return 0

    lax.fori_loop(0, nodes // 8, ends, 0)
    place = lax.broadcasted_iota(jnp.int32, (nodes, per, nodes), 0)
    at = lax.broadcasted_iota(jnp.int32, (nodes, per, nodes), 2)
    keep = place == at

    def dots(g, _):
        for k in range(8):
            node = g * 8 + k
            got = pick(src_ref[g, :, k : k + 1], node).reshape(nodes, per, width)
            sums = jnp.sum(got * ends_ref[:, node], axis=2, keepdims=True)
            out_ref[node] = jnp.sum(jnp.where(keep, sums, 0.0), axis=0) * scale
        return 0

    lax.fori_loop(0, nodes // 8, dots, 0)


def hub(rows, src_ids, dst_ids, scale):
    nodes, blocks, width = rows.shape
    edges = src_ids.shape[1]
    per = edges // nodes
    return pl.pallas_call(
        functools.partial(hub_kernel, scale),
        in_specs=[VMEM] * 3,
        out_specs=VMEM,
        out_shape=jax.ShapeDtypeStruct((nodes, per, nodes), jnp.float32),
        scratch_shapes=[pltpu.VMEM((nodes, nodes, per, width), jnp.float32)],
        compiler_params=pltpu.CompilerParams(vmem_limit_bytes=48 * 2**20),
        cost_estimate=pl.CostEstimate(
            flops=4 * nodes * edges * blocks * width, bytes_accessed=8 * 2**20, transcendentals=0
        ),
        name="hub",
    )(rows, src_ids, dst_ids)


def neg_kernel(scale, embed_ref, pool_ref, src_ref, pick_ref, out_ref):
    slots = out_ref.shape[0]
    rows = pool_ref.shape[1]

    def step(j, _):
        score = lax.dot_general(
            pool_ref[pick_ref[j]],
            embed_ref[src_ref[j]],
            (((1,), (1,)), ((), ())),
            preferred_element_type=jnp.float32,
        )
        v = score * scale
        soft = jnp.maximum(v, 0.0) + jnp.log1p(jnp.exp(-jnp.abs(v)))
        out_ref[pl.ds(j, 1), :] = jnp.sum(soft, axis=0, keepdims=True) * (1.0 / rows)
        return 0

    lax.fori_loop(0, slots, step, 0)


def neg_means(embed, pool, src, pick, scale):
    slots = src.shape[0]
    width = pool.shape[2]
    return pl.pallas_call(
        functools.partial(neg_kernel, scale),
        in_specs=[VMEM, VMEM, SMEM, SMEM],
        out_specs=VMEM,
        out_shape=jax.ShapeDtypeStruct((slots, BLK), jnp.float32),
        compiler_params=pltpu.CompilerParams(vmem_limit_bytes=32 * 2**20),
        cost_estimate=pl.CostEstimate(
            flops=slots * 2 * BLK * BLK * width,
            bytes_accessed=20 * 2**20,
            transcendentals=2 * slots * BLK * BLK,
        ),
        name="neg",
    )(embed, pool, src, pick)


def shards(nodes, reps, features, w_in, w_out, pos_src, pos_dst, counts, neg_blocks, neg_pick):
    total, width = features.shape
    blocks = total // BLK
    slots = pos_dst.shape[3]
    scale = 1.0 / width**0.5
    offered = jnp.concatenate(
        [
            lax.dynamic_slice_in_dim(features, neg_blocks[0, k] * BLK, BLK, 0)
            for k in range(neg_blocks.shape[1])
        ]
    )
    pool = lax.all_gather(
        encode(offered, w_in, w_out).reshape(-1, BLK, width), "node", axis=0, tiled=True
    )
    sent = rows_of_blocks(features, w_in, w_out, reps).reshape(nodes, blocks, width // 2)
    mine = lax.all_to_all(sent, "node", split_axis=0, concat_axis=0, tiled=True)

    own = jnp.stack([pos_src.reshape(nodes, slots), pos_dst.reshape(nodes, slots)])
    ids = lax.all_gather(own, ALL, axis=0, tiled=False).reshape(nodes, reps, 2, nodes, slots)

    def columns(t):
        t = t.reshape(nodes // 8, 8, nodes * reps * slots)
        return jnp.swapaxes(t, 1, 2)

    src_ids = columns(jnp.transpose(ids[:, :, 0], (0, 2, 1, 3)))
    dst_ids = columns(jnp.transpose(ids[:, :, 1], (2, 0, 1, 3)))

    embed = encode(features, w_in, w_out).reshape(blocks, BLK, width)
    neg = neg_means(embed, pool, pos_src.reshape(-1), neg_pick.reshape(-1), scale)

    part = hub(mine, src_ids, dst_ids, scale)
    back = lax.all_to_all(
        part.reshape(nodes * reps, slots * nodes), ALL, split_axis=0, concat_axis=0, tiled=True
    )
    back = back.reshape(nodes // 2, 2, reps, slots, nodes).sum(axis=1)
    raw = jnp.transpose(back, (3, 2, 1, 0)).reshape(nodes, slots, BLK)

    live = jnp.arange(slots, dtype=jnp.int32)[None, :] < counts.reshape(nodes, 1)
    livex = live[..., None]
    pos_out = jnp.where(livex, raw, 0.0)
    neg_out = jnp.where(livex, neg.reshape(nodes, slots, BLK), 0.0)
    partial = jnp.sum(jnp.where(livex, jax.nn.softplus(-raw), 0.0)) + jnp.sum(neg_out)
    sums = lax.psum(jnp.stack([partial, jnp.sum(counts).astype(jnp.float32)]), ALL)
    loss = sums[0] / (BLK * sums[1])
    return (
        pos_out.reshape(1, 1, nodes, slots, BLK),
        neg_out.reshape(1, 1, nodes, slots, BLK),
        loss,
    )


def solution(mesh):
    n, r = mesh.shape["node"], mesh.shape["rep"]
    return jax.shard_map(
        functools.partial(shards, n, r),
        mesh=mesh,
        in_specs=(
            P("node", None),
            P(),
            P(),
            P("node", "rep", None, None),
            P("node", "rep", None, None),
            P("node", "rep", None),
            P("node", None),
            P("node", "rep", None, None),
        ),
        out_specs=(P("node", "rep", None, None, None), P("node", "rep", None, None, None), P()),
        check_vma=False,
    )
```

```python
import functools

import jax
import jax.numpy as jnp
from jax import lax
from jax.experimental import pallas as pl
from jax.experimental.pallas import tpu as pltpu
from jax.sharding import PartitionSpec as P

MESH = pl.DeviceIdType.MESH
VMEM = pl.BlockSpec(memory_space=pltpu.VMEM)
DMA = pltpu.SemaphoreType.DMA
LANES = 128
HALF = LANES // 2


def softplus(v):
    return jnp.maximum(v, 0.0) + jnp.log1p(jnp.exp(-jnp.abs(v)))


def bits(n):
    return n.bit_length() - 1


def kernel(
    dims, scale, feat, offer, w_in, w_out, own, live, pos_out, neg_out, loss_out,
    xq, stage, emb, send, recv, pool, near, ids, idc, near_v, near_s, g_src, g_dst, part, ret1, ret2, tall, ysend, yrecv,
    negp, negr, raw, tot, ly, lc, lz,
    bulk_s, bulk_r, y_s, y_r, c_s, c_r, z_s, z_r, local, chunk_sem,
):
    Z, X, C, Y = dims
    XC, N = X * C, Z * X * C
    R = Z * X
    NB, BLK, D = emb.shape
    H = D // C
    CAP = ysend.shape[1]
    RC = Y * CAP
    NEG = pool.shape[3]
    me, q = lax.axis_index("node"), lax.axis_index("rep")
    z, xc = me // XC, me % XC
    x, c = xc // C, xc % C

    def ahead(k):
        dz, dx, dc = k // XC, (k // C) % X, k % C
        return ((z + dz) % Z) * XC + ((x + dx) % X) * C + (c + dc) % C

    def behind(k):
        dz, dx, dc = k // XC, (k // C) % X, k % C
        return ((z + Z - dz) % Z) * XC + ((x + X - dx) % X) * C + (c + C - dc) % C

    def copy(src, dst, s, r, node, rep):
        return pltpu.make_async_remote_copy(
            src_ref=src, dst_ref=dst, send_sem=s, recv_sem=r, device_id=(node, rep), device_id_type=MESH
        )

    def y_stage(n, src, dst):
        return [
            copy(src((q + j) % Y), dst, y_s.at[n, j], y_r.at[n, j], me, (q + j) % Y) for j in range(1, Y)
        ]

    def c_stage(n, src, dst):
        out = []
        for k in range(1, XC):
            to = ahead(k) % XC
            out.append(copy(src(to), dst, c_s.at[n, k], c_r.at[n, k], z * XC + to, q))
        return out

    def z_stage(n, src, dst):
        out = []
        for j in range(1, Z):
            to = (z + j) % Z
            out.append(copy(src(to), dst, z_s.at[n, j], z_r.at[n, j], to * XC + xc, q))
        return out

    def start(copies):
        for each in copies:
            each.start()
        return copies

    def arrived(copies):
        for each in copies:
            each.wait_recv()

    def sent(copies):
        for each in copies:
            each.wait_send()

    def encode(v):
        h = jnp.dot(v, w_in[...], preferred_element_type=jnp.float32)
        h = (0.5 * h * (1.0 + jnp.tanh(0.5 * h))).astype(jnp.bfloat16)
        return jnp.dot(h, w_out[...], preferred_element_type=jnp.float32).astype(jnp.bfloat16)

    barrier = pltpu.get_barrier_semaphore()

    def greet(k, _):
        pl.semaphore_signal(barrier, inc=1, device_id=(ahead(k), q), device_id_type=MESH)
        return 0

    lax.fori_loop(1, N, greet, 0)
    for j in range(1, Y):
        pl.semaphore_signal(barrier, inc=1, device_id=(me, (q + j) % Y), device_id_type=MESH)

    mine = pltpu.make_async_copy(feat.at[:, pl.ds(q * R, R), :], xq, local)
    mine.start()
    slots, per = stage.shape[0], stage.shape[1]
    chunks = NB // per

    def fetch(g, slot):
        return pltpu.make_async_copy(feat.at[pl.ds(g * per, per)], stage.at[slot], chunk_sem.at[slot])

    for g in range(min(slots, chunks)):
        fetch(g, g).start()

    pool[z, x, c] = encode(offer[...]).reshape(NEG, R, D)
    tall[...] = jnp.zeros_like(tall)
    pl.semaphore_wait(barrier, N + Y - 2)
    ids_y = start(y_stage(0, lambda to: own, near.at[q]))
    pool_z = start(z_stage(0, lambda to: pool.at[z, x, c], pool.at[z, x, c]))

    mine.wait()
    G = 16 if NB % 16 == 0 else NB
    n = G * R
    i0 = lax.broadcasted_iota(jnp.int32, (n, n), 0)
    i1 = lax.broadcasted_iota(jnp.int32, (n, n), 1)
    perm = jnp.where(i1 == (i0 & (G - 1)) * R + (i0 >> bits(G)), 1.0, 0.0).astype(jnp.bfloat16)

    def rows(g, _):
        at = pl.multiple_of(g * G, G)
        e = encode(xq[pl.ds(at, G)].reshape(n, D))
        t = jnp.dot(perm, e, preferred_element_type=jnp.float32).astype(jnp.bfloat16)
        for k in range(C):
            send[:, k, pl.ds(at, G), :] = t[:, k * H : (k + 1) * H].reshape(R, G, H)
        return 0

    lax.fori_loop(0, NB // G, rows, 0)

    def bulk(k, to):
        return copy(send.at[to // C, to % C], recv.at[me], bulk_s.at[k], bulk_r.at[k], to, q)

    def bulk_go(k, _):
        bulk(k, ahead(k)).start()
        return 0

    arrived(ids_y)
    mask = own[...]
    for j in range(1, Y):
        mask = mask + near[(q + j) % Y]
    near_v[...] = mask
    ids[z, xc] = mask[0]
    scalars = pltpu.make_async_copy(near_v, near_s, local)
    scalars.start()
    ids_z = start(z_stage(1, lambda to: ids.at[z, xc], ids.at[z, xc]))
    arrived(pool_z)
    pool_x = []
    for dx in range(1, X):
        to = z * XC + ((x + dx) % X) * C + c
        pool_x.append(copy(pool.at[:, x, c], pool.at[:, x, c], c_s.at[0, dx], c_r.at[0, dx], to, q))
    start(pool_x)
    first = N * 3 // 8
    lax.fori_loop(1, first, bulk_go, 0)

    def full(g, _):
        slot = g % slots
        fetch(g, slot).wait()
        emb[pl.ds(g * per, per)] = encode(stage[slot].reshape(per * BLK, D)).reshape(per, BLK, D)

        @pl.when(g + slots < chunks)
        def _():
            fetch(g + slots, slot).start()

        return 0

    lax.fori_loop(0, chunks, full, 0)

    arrived(ids_z)
    ids_c = start(c_stage(2, lambda to: ids.at[:, xc], ids.at[:, xc]))
    arrived(pool_x)
    pool_c = []
    for dc in range(1, C):
        to = z * XC + x * C + (c + dc) % C
        pool_c.append(
            copy(pool.at[:, :, c], pool.at[:, :, c], c_s.at[1, dc], c_r.at[1, dc], to, q)
        )
    start(pool_c)
    lax.fori_loop(first, N, bulk_go, 0)
    recv[me] = send[me // C, me % C]
    scalars.wait()
    arrived(pool_c)

    def negatives(e, _):
        r, o = e >> bits(N), e & (N - 1)
        for k in range(CAP):
            s = near_s[0, r * CAP + k, o]
            p = near_s[1, r * CAP + k, o]
            node = p >> bits(NEG)
            cand = pool[
                node >> bits(XC), (node >> bits(C)) & (X - 1), node & (C - 1), p & (NEG - 1)
            ]
            v = lax.dot_general(
                cand, emb[s], (((1,), (1,)), ((), ())), preferred_element_type=jnp.float32
            )
            negp[r, pl.ds(o * CAP + k, 1), :] = jnp.sum(softplus(v * scale), axis=0, keepdims=True)
        return 0

    lax.fori_loop(0, Y * N, negatives, 0)
    neg_y = start(y_stage(1, lambda to: negp.at[to], negr.at[q]))

    arrived(ids_c)
    lane = lax.broadcasted_iota(jnp.int32, (N, LANES), 1)
    for k in range(RC):
        a = jnp.concatenate(
            [ids[i // XC, i % XC, pl.ds(k, 1), :].astype(jnp.float32) for i in range(N)], axis=0
        )
        t = jnp.swapaxes(jnp.concatenate([a] * (LANES // N), axis=0), 0, 1)[:N]
        idc[pl.ds(k, N, stride=RC), :] = jnp.where(lane < HALF, t, a)

    number = lax.broadcasted_iota(jnp.int32, (N * RC, NB), 1).astype(jnp.float32)

    def pick(ids_col, rows_in):
        hot = jnp.where(ids_col == number, 1.0, 0.0).astype(jnp.bfloat16)
        return jnp.dot(hot, rows_in, preferred_element_type=jnp.float32).astype(jnp.bfloat16)

    def gather(s):
        cols = pltpu.roll(idc[...], (LANES - s) % LANES, 1)
        g_src[s] = pick(cols[:, :1], recv[s])
        g_dst[s] = pick(cols[:, HALF : HALF + 1], recv[s])

    def gather_step(k, _):
        bulk(k, ahead(k)).wait_recv()
        gather(behind(k))
        return 0

    gather(me)
    lax.fori_loop(1, N, gather_step, 0)

    shape = (N, RC, LANES)
    keep = lax.broadcasted_iota(jnp.int32, shape, 0) == lax.broadcasted_iota(jnp.int32, shape, 2)

    def dots(h, _):
        b = g_dst[:, pl.ds(pl.multiple_of(h * 2 * RC, 2 * RC), 2 * RC), :].astype(jnp.float32)
        for k in range(2):
            i = 2 * h + k
            a = g_src[i].astype(jnp.float32).reshape(N, RC, H)
            sums = jnp.sum(a * b[:, k * RC : (k + 1) * RC], axis=2, keepdims=True)
            part[i // XC, i % XC] = jnp.sum(jnp.where(keep, sums, 0.0), axis=0)
        return 0

    lax.fori_loop(0, N // 2, dots, 0)
    back_z = start(z_stage(2, lambda to: part.at[to], ret1.at[z]))
    ret1[z] = part[z]

    arrived(neg_y)
    neg = negp[q]
    for j in range(1, Y):
        neg = neg + negr[(q + j) % Y]
    lit = live[...] > 0.0
    neg = jnp.where(lit, neg * (1.0 / BLK), 0.0)
    neg_out[...] = neg

    arrived(back_z)
    back_c = start(c_stage(3, lambda to: ret1.at[:, to], ret2.at[xc]))
    ret2[xc] = ret1[:, xc]
    arrived(back_c)
    for xx in range(X):
        v = ret2[xx * C]
        for k in range(1, C):
            v = v + ret2[xx * C + k]
        for zz in range(Z):
            at = pl.multiple_of((q * R + zz * X + xx) * RC, RC)
            tall[pl.ds(at, RC), :] = v[zz]
    for r in range(Y):
        for k in range(CAP):
            rows_b = tall[pl.ds(r * CAP + k, BLK, stride=RC), :]
            ysend[r, k] = jnp.swapaxes(rows_b, 0, 1)[:N]
    back_y = start(y_stage(2, lambda to: ysend.at[to], yrecv.at[q]))
    arrived(back_y)
    for k in range(CAP):
        v = ysend[q, k]
        for j in range(1, Y):
            v = v + yrecv[(q + j) % Y, k]
        raw[pl.ds(k, N, stride=CAP), :] = v * scale
    v = raw[...]
    pos_out[...] = jnp.where(lit, v, 0.0)
    loss = jnp.sum(jnp.where(lit, softplus(-v), 0.0) + neg)
    count = jnp.sum(live[...])
    spot = lax.broadcasted_iota(jnp.int32, tot.shape[1:], 1)
    tot[0] = jnp.where(spot == 0, loss, jnp.where(spot == 1, count, 0.0))

    add_y = start(y_stage(3, lambda to: tot.at[0], ly.at[q]))
    arrived(add_y)
    v = tot[0]
    for j in range(1, Y):
        v = v + ly[(q + j) % Y]
    tot[1] = v
    add_c = start(c_stage(4, lambda to: tot.at[1], lc.at[xc]))
    arrived(add_c)
    for k in range(1, XC):
        v = v + lc[behind(k) % XC]
    tot[2] = v
    add_z = start(z_stage(3, lambda to: tot.at[2], lz.at[z]))
    arrived(add_z)
    for j in range(1, Z):
        v = v + lz[(z + j) % Z]
    loss_out[...] = v

    for copies in (ids_y, ids_z, ids_c, pool_z, pool_x, pool_c, neg_y, back_z, back_c, back_y, add_y, add_c, add_z):
        sent(copies)

    def bulk_sent(k, _):
        bulk(k, ahead(k)).wait_send()
        return 0

    lax.fori_loop(1, N, bulk_sent, 0)


def step(dims, features, w_in, w_out, pos_src, pos_dst, counts, neg_blocks, neg_pick):
    Z, X, C, Y = dims
    XC, N, R = X * C, Z * X * C, Z * X
    total, D = features.shape
    BLK = R * Y
    NB = total // BLK
    H = D // C
    CAP = pos_dst.shape[3]
    RC = Y * CAP
    NEG = neg_blocks.shape[1]
    bf, f32, i32 = jnp.bfloat16, jnp.float32, jnp.int32
    scale = 1.0 / D**0.5
    q = lax.axis_index("rep")
    offer = jnp.concatenate(
        [lax.dynamic_slice_in_dim(features, neg_blocks[0, k] * BLK + q * R, R, 0) for k in range(NEG)]
    )

    def slab(a, b):
        pad = ((0, 0), (0, HALF - N))
        t = jnp.concatenate([jnp.pad(a.T, pad), jnp.pad(b.T, pad)], axis=1)
        t = jnp.tile(t, (Y, 1))
        return jnp.where(jnp.arange(RC)[:, None] // CAP == q, t, 0)

    src, dst, pick = (t.reshape(N, CAP) for t in (pos_src, pos_dst, neg_pick))
    own = jnp.stack([slab(src, dst), slab(pick, pick)])
    live = jnp.arange(CAP, dtype=i32)[None, :] < counts.reshape(N, 1)
    live = jnp.broadcast_to(live.astype(f32).reshape(N * CAP, 1), (N * CAP, BLK))
    per, slots = (8, 4) if NB % 8 == 0 else (NB, 1)
    scratch = [
        pltpu.VMEM((NB, R, D), bf),
        pltpu.VMEM((slots, per, BLK, D), bf),
        pltpu.VMEM((NB, BLK, D), bf),
        pltpu.VMEM((R, C, NB, H), bf),
        pltpu.VMEM((N, NB, H), bf),
        pltpu.VMEM((Z, X, C, NEG, R, D), bf),
        pltpu.VMEM((Y, 2, RC, LANES), i32),
        pltpu.VMEM((Z, XC, RC, LANES), i32),
        pltpu.VMEM((N * RC, LANES), f32),
        pltpu.VMEM((2, RC, LANES), i32),
        pltpu.SMEM((2, RC, LANES), i32),
        pltpu.VMEM((N, N * RC, H), bf),
        pltpu.VMEM((N, N * RC, H), bf),
        pltpu.VMEM((Z, XC, RC, LANES), f32),
        pltpu.VMEM((Z, XC, RC, LANES), f32),
        pltpu.VMEM((XC, Z, RC, LANES), f32),
        pltpu.VMEM((BLK * RC, LANES), f32),
        pltpu.VMEM((Y, CAP, N, BLK), f32),
        pltpu.VMEM((Y, CAP, N, BLK), f32),
        pltpu.VMEM((Y, N * CAP, BLK), f32),
        pltpu.VMEM((Y, N * CAP, BLK), f32),
        pltpu.VMEM((N * CAP, BLK), f32),
        pltpu.VMEM((3, 8, LANES), f32),
        pltpu.VMEM((Y, 8, LANES), f32),
        pltpu.VMEM((XC, 8, LANES), f32),
        pltpu.VMEM((Z, 8, LANES), f32),
        DMA((N,)),
        DMA((N,)),
        DMA((4, Y)),
        DMA((4, Y)),
        DMA((5, XC)),
        DMA((5, XC)),
        DMA((4, Z)),
        DMA((4, Z)),
        DMA,
        DMA((slots,)),
    ]
    pos, neg, sums = pl.pallas_call(
        functools.partial(kernel, dims, scale),
        in_specs=[pl.BlockSpec(memory_space=pl.ANY)] + [VMEM] * 5,
        out_specs=[VMEM] * 3,
        out_shape=[
            jax.ShapeDtypeStruct((N * CAP, BLK), f32),
            jax.ShapeDtypeStruct((N * CAP, BLK), f32),
            jax.ShapeDtypeStruct((8, LANES), f32),
        ],
        scratch_shapes=scratch,
        compiler_params=pltpu.CompilerParams(
            collective_id=0, has_side_effects=True, vmem_limit_bytes=60 * 2**20
        ),
        name="step",
    )(features.reshape(NB, BLK, D), offer, w_in, w_out, own, live)
    loss = sums[0, 0] / sums[0, 1]
    shape = (1, 1, N, CAP, BLK)
    return pos.reshape(shape), neg.reshape(shape), loss


def solution(mesh):
    n, reps = mesh.shape["node"], mesh.shape["rep"]
    dims = (n // 8, 4, 2, reps) if n >= 32 else (n // 4, 2, 2, reps)
    return jax.shard_map(
        functools.partial(step, dims),
        mesh=mesh,
        in_specs=(
            P("node", None),
            P(),
            P(),
            P("node", "rep", None, None),
            P("node", "rep", None, None),
            P("node", "rep", None),
            P("node", None),
            P("node", "rep", None, None),
        ),
        out_specs=(P("node", "rep", None, None, None), P("node", "rep", None, None, None), P()),
        check_vma=False,
    )
```

```python
import functools

import jax
import jax.numpy as jnp
from jax import lax
from jax.experimental import pallas as pl
from jax.experimental.pallas import tpu as pltpu
from jax.sharding import PartitionSpec as P

MESH = pl.DeviceIdType.MESH
VMEM = pl.BlockSpec(memory_space=pltpu.VMEM)
DMA = pltpu.SemaphoreType.DMA
LANES = 128
HALF = LANES // 2


def softplus(v):
    return jnp.maximum(v, 0.0) + jnp.log1p(jnp.exp(-jnp.abs(v)))


def bits(n):
    return n.bit_length() - 1


def kernel(
    dims, scale, feat, chosen, w_in, w_out, own, pos_out, neg_out, loss_out,
    xq, stage, emb, send, recv, pool, near, ids, idc, near_v, near_s, ends, part, other, half, ret, tall, ysend, yrecv,
    negp, negr, tot, lp, ly,
    bulk_s, bulk_r, back_s, back_r, loss_s, loss_r, y_s, y_r, c_s, c_r, z_s, z_r, die, local, chunk_sem,
):
    Z, X, C, Y = dims
    XC, N = X * C, Z * X * C
    R = Z * X
    NB, BLK, D = emb.shape
    H = D // C
    CAP = ysend.shape[1]
    RC = Y * CAP
    NEG = pool.shape[3]
    me, q = lax.axis_index("node"), lax.axis_index("rep")
    z, xc = me // XC, me % XC
    x, c = xc // C, xc % C

    def ahead(k):
        dz, dx, dc = k // XC, (k // C) % X, k % C
        return ((z + dz) % Z) * XC + ((x + dx) % X) * C + (c + dc) % C

    def behind(k):
        dz, dx, dc = k // XC, (k // C) % X, k % C
        return ((z + Z - dz) % Z) * XC + ((x + X - dx) % X) * C + (c + C - dc) % C

    def copy(src, dst, s, r, node, rep):
        return pltpu.make_async_remote_copy(
            src_ref=src, dst_ref=dst, send_sem=s, recv_sem=r, device_id=(node, rep), device_id_type=MESH
        )

    def y_stage(n, src, dst):
        return [
            copy(src((q + j) % Y), dst, y_s.at[n, j], y_r.at[n, j], me, (q + j) % Y) for j in range(1, Y)
        ]

    def c_stage(n, src, dst):
        out = []
        for k in range(1, XC):
            to = ahead(k) % XC
            out.append(copy(src(to), dst, c_s.at[n, k], c_r.at[n, k], z * XC + to, q))
        return out

    def z_stage(n, src, dst):
        out = []
        for j in range(1, Z):
            to = (z + j) % Z
            out.append(copy(src(to), dst, z_s.at[n, j], z_r.at[n, j], to * XC + xc, q))
        return out

    def start(copies):
        for each in copies:
            each.start()
        return copies

    def arrived(copies):
        for each in copies:
            each.wait_recv()

    def sent(copies):
        for each in copies:
            each.wait_send()

    def encode(v):
        h = jnp.dot(v, w_in[...], preferred_element_type=jnp.float32)
        h = (0.5 * h * (1.0 + jnp.tanh(0.5 * h))).astype(jnp.bfloat16)
        return jnp.dot(h, w_out[...], preferred_element_type=jnp.float32).astype(jnp.bfloat16)

    barrier = pltpu.get_barrier_semaphore()

    def greet(k, _):
        pl.semaphore_signal(barrier, inc=1, device_id=(ahead(k), q), device_id_type=MESH)
        return 0

    lax.fori_loop(1, N, greet, 0)
    for j in range(1, Y):
        pl.semaphore_signal(barrier, inc=1, device_id=(me, (q + j) % Y), device_id_type=MESH)

    mine = pltpu.make_async_copy(feat.at[:, pl.ds(q * R, R), :], xq, local)
    mine.start()
    slots, per = stage.shape[0], stage.shape[1]
    chunks = NB // per

    def fetch(g, slot):
        return pltpu.make_async_copy(feat.at[pl.ds(g * per, per)], stage.at[slot], chunk_sem.at[slot])

    for g in range(min(slots, chunks)):
        fetch(g, g).start()

    tall[...] = jnp.zeros_like(tall)
    fill = lax.broadcasted_iota(jnp.int32, (2, RC, LANES), 1) // CAP == q
    near_v[...] = jnp.where(fill, jnp.concatenate([own[...]] * Y, axis=1), 0)
    mine.wait()
    offer = jnp.concatenate([xq[chosen[0, k]] for k in range(NEG)], axis=0)
    pool[z, x, c] = encode(offer).reshape(NEG, R, D)
    pl.semaphore_wait(barrier, N + Y - 2)
    ids_y = start(y_stage(0, lambda to: near_v, near.at[q]))
    pool_z = start(z_stage(0, lambda to: pool.at[z, x, c], pool.at[z, x, c]))

    G = 16 if NB % 16 == 0 else NB
    n = G * R
    i0 = lax.broadcasted_iota(jnp.int32, (n, n), 0)
    i1 = lax.broadcasted_iota(jnp.int32, (n, n), 1)
    perm = jnp.where(i1 == (i0 & (G - 1)) * R + (i0 >> bits(G)), 1.0, 0.0).astype(jnp.bfloat16)

    def rows(g, _):
        at = pl.multiple_of(g * G, G)
        e = encode(xq[pl.ds(at, G)].reshape(n, D))
        t = jnp.dot(perm, e, preferred_element_type=jnp.float32).astype(jnp.bfloat16)
        for k in range(C):
            send[:, k, pl.ds(at, G), :] = t[:, k * H : (k + 1) * H].reshape(R, G, H)
        return 0

    lax.fori_loop(0, NB // G, rows, 0)

    def bulk(k):
        to = ahead(k)
        return copy(send.at[to // C, to % C], recv.at[me], bulk_s.at[k], bulk_r.at[k], to, q)

    def bulk_go(k, _):
        bulk(k).start()
        return 0

    arrived(ids_y)
    tile = near_v[...]
    for j in range(1, Y):
        tile = tile + near[(q + j) % Y]
    near[q] = tile
    ids[z, xc] = tile[0]
    ids_z = start(z_stage(1, lambda to: ids.at[z, xc], ids.at[z, xc]))
    scalars = pltpu.make_async_copy(near.at[q], near_s, local)
    scalars.start()
    arrived(pool_z)
    pool_x = []
    for dx in range(1, X):
        to = z * XC + ((x + dx) % X) * C + c
        pool_x.append(copy(pool.at[:, x, c], pool.at[:, x, c], c_s.at[0, dx], c_r.at[0, dx], to, q))
    start(pool_x)
    first = N // 4
    lax.fori_loop(1, first, bulk_go, 0)

    def full(g, _):
        slot = g % slots
        fetch(g, slot).wait()
        emb[pl.ds(g * per, per)] = encode(stage[slot].reshape(per * BLK, D)).reshape(per, BLK, D)

        @pl.when(g + slots < chunks)
        def _():
            fetch(g + slots, slot).start()

        return 0

    lax.fori_loop(0, chunks, full, 0)

    arrived(ids_z)
    ids_c = start(c_stage(2, lambda to: ids.at[:, xc], ids.at[:, xc]))
    arrived(pool_x)
    pool_c = []
    for dc in range(1, C):
        to = z * XC + x * C + (c + dc) % C
        pool_c.append(
            copy(pool.at[:, :, c], pool.at[:, :, c], c_s.at[1, dc], c_r.at[1, dc], to, q)
        )
    start(pool_c)
    lax.fori_loop(first, N, bulk_go, 0)
    recv[me] = send[me // C, me % C]
    scalars.wait()
    arrived(pool_c)

    def negatives(e, _):
        for k in range(2 * CAP):
            r, o = e >> bits(N // 2), (e & (N // 2 - 1)) * 2 + k // CAP
            s = near_s[0, r * CAP + k % CAP, o]
            p = near_s[1, r * CAP + k % CAP, o]
            node = p >> bits(NEG)
            cand = pool[
                node >> bits(XC), (node >> bits(C)) & (X - 1), node & (C - 1), p & (NEG - 1)
            ]
            v = lax.dot_general(
                cand,
                emb[jnp.maximum(s, 0)],
                (((1,), (1,)), ((), ())),
                preferred_element_type=jnp.float32,
            )
            total = jnp.sum(softplus(v * scale), axis=0, keepdims=True)
            negp[r, pl.ds(o * CAP + k % CAP, 1), :] = jnp.where(s >= 0, total, 0.0)
        return 0

    lax.fori_loop(0, Y * N // 2, negatives, 0)
    neg_y = start(y_stage(1, lambda to: negp.at[to], negr.at[q]))

    arrived(ids_c)
    lane = lax.broadcasted_iota(jnp.int32, (N, LANES), 1)
    for k in range(RC):
        a = jnp.concatenate(
            [ids[i // XC, i % XC, pl.ds(k, 1), :].astype(jnp.float32) for i in range(N)], axis=0
        )
        t = jnp.swapaxes(jnp.concatenate([a] * (LANES // N), axis=0), 0, 1)[:N]
        idc[pl.ds(k, N, stride=RC), :] = jnp.where(lane < HALF, t, a)

    number = lax.broadcasted_iota(jnp.int32, (2 * N * RC, NB), 1).astype(jnp.float32)

    def gather(s):
        cols = pltpu.roll(idc[...], (LANES - s) % LANES, 1)
        col = jnp.concatenate([cols[:, :1], cols[:, HALF : HALF + 1]], axis=0)
        hot = jnp.where(col == number, 1.0, 0.0).astype(jnp.bfloat16)
        got = jnp.dot(hot, recv[s], preferred_element_type=jnp.float32).astype(jnp.bfloat16)
        ends[s] = got.reshape(2, N * RC, H)

    def gather_step(k, _):
        bulk(k).wait_recv()
        gather(behind(k))
        return 0

    gather(me)
    lax.fori_loop(1, N, gather_step, 0)

    shape = (N, RC, LANES)
    keep = lax.broadcasted_iota(jnp.int32, shape, 0) == lax.broadcasted_iota(jnp.int32, shape, 2)

    def dots(h, _):
        at = pl.multiple_of(h * 2 * RC, 2 * RC)
        b = ends[:, 1, pl.ds(at, 2 * RC), :].astype(jnp.float32)
        for k in range(2):
            i = 2 * h + k
            a = ends[i, 0].astype(jnp.float32).reshape(N, RC, H)
            sums = jnp.sum(a * b[:, k * RC : (k + 1) * RC], axis=2, keepdims=True)
            part[i // XC, (i % XC) // C, i % C] = jnp.sum(jnp.where(keep, sums, 0.0), axis=0)
        return 0

    lax.fori_loop(0, N // 2, dots, 0)

    to = z * XC + x * C + (c + 1) % C
    swap = copy(part.at[:, :, (c + 1) % C], other, die.at[0], die.at[1], to, q)
    swap.start()
    arrived(neg_y)
    neg = negp[q]
    for j in range(1, Y):
        neg = neg + negr[(q + j) % Y]
    neg = neg * (1.0 / BLK)
    neg_out[...] = neg
    loss = jnp.sum(neg)
    edge = lax.broadcasted_iota(jnp.int32, (CAP, LANES), 1) < N
    count = jnp.sum(jnp.where(edge & (own[0] >= 0), 1.0, 0.0)) * BLK
    swap.wait_recv()
    v = (part[:, :, c] + other[...]) * scale
    half[...] = v

    def back(k):
        to = ((z + k // X) % Z) * XC + ((x + k % X) % X) * C + c
        return copy(half.at[to // XC, (to % XC) // C], ret.at[z, x], back_s.at[k], back_r.at[k], to, q)

    def back_go(k, _):
        back(k).start()
        return 0

    def back_got(k, _):
        back(k).wait_recv()
        return 0

    lax.fori_loop(1, R, back_go, 0)
    lit = jnp.concatenate([ids[:, k * C + c][:, None] for k in range(X)], axis=1) >= 0
    lit = lit & (lax.broadcasted_iota(jnp.int32, (Z, X, RC, LANES), 3) < N)
    loss = loss + jnp.sum(jnp.where(lit, softplus(-v), 0.0))
    spot = lax.broadcasted_iota(jnp.int32, tot.shape[1:], 1)
    mine_sum = jnp.where(spot == 0, loss, jnp.where(spot == 1, count, 0.0))
    tot[0] = mine_sum
    ret[z, x] = half[z, x]

    def add(k):
        return copy(tot.at[0], lp.at[me], loss_s.at[k], loss_r.at[k], ahead(k), q)

    def add_go(k, _):
        add(k).start()
        return 0

    def add_got(k, v):
        add(k).wait_recv()
        return v + lp[behind(k)]

    lax.fori_loop(1, N, add_go, 0)
    lax.fori_loop(1, R, back_got, 0)
    for k in range(R):
        at = pl.multiple_of((q * R + k) * RC, RC)
        tall[pl.ds(at, RC), :] = ret[k // X, k % X]
    for r in range(Y):
        for k in range(CAP):
            rows_b = tall[pl.ds(r * CAP + k, BLK, stride=RC), :]
            ysend[r, k] = jnp.swapaxes(rows_b, 0, 1)[:N]
    back_y = start(y_stage(2, lambda to: ysend.at[to], yrecv.at[q]))
    total = lax.fori_loop(1, N, add_got, mine_sum)
    tot[1] = total
    add_y = start(y_stage(3, lambda to: tot.at[1], ly.at[q]))
    arrived(back_y)
    for k in range(CAP):
        v = ysend[q, k]
        for j in range(1, Y):
            v = v + yrecv[(q + j) % Y, k]
        pos_out[pl.ds(k, N, stride=CAP), :] = v
    arrived(add_y)
    for j in range(1, Y):
        total = total + ly[(q + j) % Y]
    loss_out[...] = total

    for copies in (ids_y, ids_z, ids_c, pool_z, pool_x, pool_c, neg_y, back_y, add_y):
        sent(copies)
    swap.wait_send()

    def bulk_sent(k, _):
        bulk(k).wait_send()
        add(k).wait_send()
        return 0

    def back_sent(k, _):
        back(k).wait_send()
        return 0

    lax.fori_loop(1, N, bulk_sent, 0)
    lax.fori_loop(1, R, back_sent, 0)


def step(dims, features, w_in, w_out, pos_src, pos_dst, counts, neg_blocks, neg_pick):
    Z, X, C, Y = dims
    XC, N, R = X * C, Z * X * C, Z * X
    total, D = features.shape
    BLK = R * Y
    NB = total // BLK
    H = D // C
    CAP = pos_dst.shape[3]
    RC = Y * CAP
    NEG = neg_blocks.shape[1]
    bf, f32, i32 = jnp.bfloat16, jnp.float32, jnp.int32
    scale = 1.0 / D**0.5
    src, dst, pick = (t.reshape(N, CAP) for t in (pos_src, pos_dst, neg_pick))
    live = jnp.arange(CAP, dtype=i32)[None, :] < counts.reshape(N, 1)
    own = jnp.stack([jnp.where(live, src, -1), dst, pick, pick])
    own = jnp.transpose(own.reshape(2, 2, N, CAP), (0, 3, 1, 2))
    own = jnp.pad(own, ((0, 0), (0, 0), (0, 0), (0, HALF - N))).reshape(2, CAP, LANES)
    per, slots = (8, 4) if NB % 8 == 0 else (NB, 1)
    scratch = [
        pltpu.VMEM((NB, R, D), bf),
        pltpu.VMEM((slots, per, BLK, D), bf),
        pltpu.VMEM((NB, BLK, D), bf),
        pltpu.VMEM((R, C, NB, H), bf),
        pltpu.VMEM((N, NB, H), bf),
        pltpu.VMEM((Z, X, C, NEG, R, D), bf),
        pltpu.VMEM((Y, 2, RC, LANES), i32),
        pltpu.VMEM((Z, XC, RC, LANES), i32),
        pltpu.VMEM((N * RC, LANES), f32),
        pltpu.VMEM((2, RC, LANES), i32),
        pltpu.SMEM((2, RC, LANES), i32),
        pltpu.VMEM((N, 2, N * RC, H), bf),
        pltpu.VMEM((Z, X, C, RC, LANES), f32),
        pltpu.VMEM((Z, X, RC, LANES), f32),
        pltpu.VMEM((Z, X, RC, LANES), f32),
        pltpu.VMEM((Z, X, RC, LANES), f32),
        pltpu.VMEM((BLK * RC, LANES), f32),
        pltpu.VMEM((Y, CAP, N, BLK), f32),
        pltpu.VMEM((Y, CAP, N, BLK), f32),
        pltpu.VMEM((Y, N * CAP, BLK), f32),
        pltpu.VMEM((Y, N * CAP, BLK), f32),
        pltpu.VMEM((2, 8, LANES), f32),
        pltpu.VMEM((N, 8, LANES), f32),
        pltpu.VMEM((Y, 8, LANES), f32),
        DMA((N,)),
        DMA((N,)),
        DMA((R,)),
        DMA((R,)),
        DMA((N,)),
        DMA((N,)),
        DMA((4, Y)),
        DMA((4, Y)),
        DMA((3, XC)),
        DMA((3, XC)),
        DMA((2, Z)),
        DMA((2, Z)),
        DMA((2,)),
        DMA,
        DMA((slots,)),
    ]
    pos, neg, sums = pl.pallas_call(
        functools.partial(kernel, dims, scale),
        in_specs=[pl.BlockSpec(memory_space=pl.ANY), pl.BlockSpec(memory_space=pltpu.SMEM)] + [VMEM] * 3,
        out_specs=[VMEM] * 3,
        out_shape=[
            jax.ShapeDtypeStruct((N * CAP, BLK), f32),
            jax.ShapeDtypeStruct((N * CAP, BLK), f32),
            jax.ShapeDtypeStruct((8, LANES), f32),
        ],
        scratch_shapes=scratch,
        compiler_params=pltpu.CompilerParams(
            collective_id=0, has_side_effects=True, vmem_limit_bytes=60 * 2**20
        ),
        name="step",
    )(features.reshape(NB, BLK, D), neg_blocks, w_in, w_out, own)
    loss = sums[0, 0] / sums[0, 1]
    shape = (1, 1, N, CAP, BLK)
    return pos.reshape(shape), neg.reshape(shape), loss


def solution(mesh):
    n, reps = mesh.shape["node"], mesh.shape["rep"]
    dims = (n // 8, 4, 2, reps) if n >= 32 else (n // 4, 2, 2, reps)
    return jax.shard_map(
        functools.partial(step, dims),
        mesh=mesh,
        in_specs=(
            P("node", None),
            P(),
            P(),
            P("node", "rep", None, None),
            P("node", "rep", None, None),
            P("node", "rep", None),
            P("node", None),
            P("node", "rep", None, None),
        ),
        out_specs=(P("node", "rep", None, None, None), P("node", "rep", None, None, None), P()),
        check_vma=False,
    )
```

```python
import functools

import jax
import jax.numpy as jnp
from jax import lax
from jax.experimental import pallas as pl
from jax.experimental.pallas import tpu as pltpu
from jax.sharding import PartitionSpec as P

MESH = pl.DeviceIdType.MESH
VMEM = pl.BlockSpec(memory_space=pltpu.VMEM)
DMA = pltpu.SemaphoreType.DMA
LANES = 128
HALF = LANES // 2


def softplus(v):
    return jnp.maximum(v, 0.0) + jnp.log1p(jnp.exp(-jnp.abs(v)))


def bits(n):
    return n.bit_length() - 1


def kernel(
    dims, scale, feat, chosen, w_in, w_out, own, pos_out, neg_out, loss_out,
    xq, stage, emb, send, recv, pool, near, ids, idc, near_v, near_s, ends, part, other, half, ret, tall, ysend, yrecv,
    negp, negr, tot, lc, lz, ly,
    bulk_s, bulk_r, back_s, back_r, y_s, y_r, c_s, c_r, z_s, z_r, die, local, chunk_sem,
):
    Z, X, C, Y = dims
    XC, N = X * C, Z * X * C
    R = Z * X
    NB, BLK, D = emb.shape
    H = D // C
    CAP = ysend.shape[1]
    RC = Y * CAP
    NEG = pool.shape[3]
    me, q = lax.axis_index("node"), lax.axis_index("rep")
    z, xc = me // XC, me % XC
    x, c = xc // C, xc % C

    def ahead(k):
        dz, dx, dc = k // XC, (k // C) % X, k % C
        return ((z + dz) % Z) * XC + ((x + dx) % X) * C + (c + dc) % C

    def behind(k):
        dz, dx, dc = k // XC, (k // C) % X, k % C
        return ((z + Z - dz) % Z) * XC + ((x + X - dx) % X) * C + (c + C - dc) % C

    def copy(src, dst, s, r, node, rep):
        return pltpu.make_async_remote_copy(
            src_ref=src, dst_ref=dst, send_sem=s, recv_sem=r, device_id=(node, rep), device_id_type=MESH
        )

    def y_stage(n, src, dst):
        return [
            copy(src((q + j) % Y), dst, y_s.at[n, j], y_r.at[n, j], me, (q + j) % Y) for j in range(1, Y)
        ]

    def c_stage(n, src, dst):
        out = []
        for k in range(1, XC):
            to = ahead(k) % XC
            out.append(copy(src(to), dst, c_s.at[n, k], c_r.at[n, k], z * XC + to, q))
        return out

    def z_stage(n, src, dst):
        out = []
        for j in range(1, Z):
            to = (z + j) % Z
            out.append(copy(src(to), dst, z_s.at[n, j], z_r.at[n, j], to * XC + xc, q))
        return out

    def start(copies):
        for each in copies:
            each.start()
        return copies

    def arrived(copies):
        for each in copies:
            each.wait_recv()

    def sent(copies):
        for each in copies:
            each.wait_send()

    def encode(v):
        h = jnp.dot(v, w_in[...], preferred_element_type=jnp.float32)
        h = (0.5 * h * (1.0 + jnp.tanh(0.5 * h))).astype(jnp.bfloat16)
        return jnp.dot(h, w_out[...], preferred_element_type=jnp.float32).astype(jnp.bfloat16)

    barrier = pltpu.get_barrier_semaphore()

    def greet(k, _):
        pl.semaphore_signal(barrier, inc=1, device_id=(ahead(k), q), device_id_type=MESH)
        return 0

    lax.fori_loop(1, XC, greet, 0)
    for j in range(1, Z):
        to = ((z + j) % Z) * XC + xc
        pl.semaphore_signal(barrier, inc=1, device_id=(to, q), device_id_type=MESH)
    for j in range(1, Y):
        pl.semaphore_signal(barrier, inc=1, device_id=(me, (q + j) % Y), device_id_type=MESH)

    mine = pltpu.make_async_copy(feat.at[:, pl.ds(q * R, R), :], xq, local)
    mine.start()
    slots, per = stage.shape[0], stage.shape[1]
    chunks = NB // per

    def fetch(g, slot):
        return pltpu.make_async_copy(feat.at[pl.ds(g * per, per)], stage.at[slot], chunk_sem.at[slot])

    for g in range(min(slots, chunks)):
        fetch(g, g).start()

    tall[...] = jnp.zeros_like(tall)
    fill = lax.broadcasted_iota(jnp.int32, (2, RC, LANES), 1) // CAP == q
    near_v[...] = jnp.where(fill, jnp.concatenate([own[...]] * Y, axis=1), 0)
    mine.wait()
    offer = jnp.concatenate([xq[chosen[0, k]] for k in range(NEG)], axis=0)
    pool[z, x, c] = encode(offer).reshape(NEG, R, D)
    pl.semaphore_wait(barrier, XC + Z + Y - 3)
    ids_y = start(y_stage(0, lambda to: near_v, near.at[q]))
    pool_z = start(z_stage(0, lambda to: pool.at[z, x, c], pool.at[z, x, c]))

    G = 16 if NB % 16 == 0 else NB
    n = G * R
    i0 = lax.broadcasted_iota(jnp.int32, (n, n), 0)
    i1 = lax.broadcasted_iota(jnp.int32, (n, n), 1)
    perm = jnp.where(i1 == (i0 & (G - 1)) * R + (i0 >> bits(G)), 1.0, 0.0).astype(jnp.bfloat16)

    def rows(g, _):
        at = pl.multiple_of(g * G, G)
        e = encode(xq[pl.ds(at, G)].reshape(n, D))
        t = jnp.dot(perm, e, preferred_element_type=jnp.float32).astype(jnp.bfloat16)
        for k in range(C):
            send[:, k, pl.ds(at, G), :] = t[:, k * H : (k + 1) * H].reshape(R, G, H)
        return 0

    lax.fori_loop(0, NB // G, rows, 0)

    def bulk(k):
        to = ahead(k)
        return copy(send.at[to // C, to % C], recv.at[me], bulk_s.at[k], bulk_r.at[k], to, q)

    def column(m):
        return bulk((m // C) * XC + m % C)

    side = (X - 1) * C

    def others(m):
        return bulk((m // side) * XC + C + m % side)

    def column_go(m, _):
        column(m).start()
        return 0

    def others_go(m, _):
        others(m).start()
        return 0

    arrived(ids_y)
    tile = near_v[...]
    for j in range(1, Y):
        tile = tile + near[(q + j) % Y]
    near[q] = tile
    ids[z, xc] = tile[0]
    ids_z = start(z_stage(1, lambda to: ids.at[z, xc], ids.at[z, xc]))
    scalars = pltpu.make_async_copy(near.at[q], near_s, local)
    scalars.start()
    arrived(pool_z)
    pool_x = []
    for dx in range(1, X):
        to = z * XC + ((x + dx) % X) * C + c
        pool_x.append(copy(pool.at[:, x, c], pool.at[:, x, c], c_s.at[0, dx], c_r.at[0, dx], to, q))
    start(pool_x)
    lax.fori_loop(1, Z * C, column_go, 0)
    recv[me] = send[me // C, me % C]

    def full(g, _):
        slot = g % slots
        fetch(g, slot).wait()
        emb[pl.ds(g * per, per)] = encode(stage[slot].reshape(per * BLK, D)).reshape(per, BLK, D)

        @pl.when(g + slots < chunks)
        def _():
            fetch(g + slots, slot).start()

        return 0

    lax.fori_loop(0, chunks // 4, full, 0)
    arrived(ids_z)
    ids_c = start(c_stage(2, lambda to: ids.at[:, xc], ids.at[:, xc]))
    lax.fori_loop(chunks // 4, chunks, full, 0)
    arrived(pool_x)
    pool_c = []
    for dc in range(1, C):
        to = z * XC + x * C + (c + dc) % C
        pool_c.append(
            copy(pool.at[:, :, c], pool.at[:, :, c], c_s.at[1, dc], c_r.at[1, dc], to, q)
        )
    start(pool_c)
    lax.fori_loop(0, Z * side, others_go, 0)
    scalars.wait()
    arrived(pool_c)

    def negatives(e, _):
        for k in range(2 * CAP):
            r, o = e >> bits(N // 2), (e & (N // 2 - 1)) * 2 + k // CAP
            s = near_s[0, r * CAP + k % CAP, o]
            p = near_s[1, r * CAP + k % CAP, o]
            node = p >> bits(NEG)
            cand = pool[
                node >> bits(XC), (node >> bits(C)) & (X - 1), node & (C - 1), p & (NEG - 1)
            ]
            v = lax.dot_general(
                cand,
                emb[jnp.maximum(s, 0)],
                (((1,), (1,)), ((), ())),
                preferred_element_type=jnp.float32,
            )
            total = jnp.sum(softplus(v * scale), axis=0, keepdims=True)
            negp[r, pl.ds(o * CAP + k % CAP, 1), :] = jnp.where(s >= 0, total, 0.0)
        return 0

    lax.fori_loop(0, Y * N // 2, negatives, 0)
    neg_y = start(y_stage(1, lambda to: negp.at[to], negr.at[q]))

    arrived(ids_c)
    lane = lax.broadcasted_iota(jnp.int32, (N, LANES), 1)
    for k in range(RC):
        a = jnp.concatenate(
            [ids[i // XC, i % XC, pl.ds(k, 1), :].astype(jnp.float32) for i in range(N)], axis=0
        )
        t = jnp.swapaxes(jnp.concatenate([a] * (LANES // N), axis=0), 0, 1)[:N]
        idc[pl.ds(k, N, stride=RC), :] = jnp.where(lane < HALF, t, a)

    number = lax.broadcasted_iota(jnp.int32, (2 * N * RC, NB), 1).astype(jnp.float32)

    def gather(s):
        cols = pltpu.roll(idc[...], (LANES - s) % LANES, 1)
        col = jnp.concatenate([cols[:, :1], cols[:, HALF : HALF + 1]], axis=0)
        hot = jnp.where(col == number, 1.0, 0.0).astype(jnp.bfloat16)
        got = jnp.dot(hot, recv[s], preferred_element_type=jnp.float32).astype(jnp.bfloat16)
        ends[s] = got.reshape(2, N * RC, H)

    def gather_column(m, _):
        column(m).wait_recv()
        gather(behind((m // C) * XC + m % C))
        return 0

    def gather_others(m, _):
        others(m).wait_recv()
        gather(behind((m // side) * XC + C + m % side))
        return 0

    gather(me)
    lax.fori_loop(1, Z * C, gather_column, 0)
    lax.fori_loop(0, Z * side, gather_others, 0)

    shape = (N, RC, LANES)
    keep = lax.broadcasted_iota(jnp.int32, shape, 0) == lax.broadcasted_iota(jnp.int32, shape, 2)

    def dots(h, _):
        at = pl.multiple_of(h * 2 * RC, 2 * RC)
        b = ends[:, 1, pl.ds(at, 2 * RC), :].astype(jnp.float32)
        for k in range(2):
            i = 2 * h + k
            a = ends[i, 0].astype(jnp.float32).reshape(N, RC, H)
            sums = jnp.sum(a * b[:, k * RC : (k + 1) * RC], axis=2, keepdims=True)
            part[i // XC, (i % XC) // C, i % C] = jnp.sum(jnp.where(keep, sums, 0.0), axis=0)
        return 0

    lax.fori_loop(0, N // 2, dots, 0)

    to = z * XC + x * C + (c + 1) % C
    swap = copy(part.at[:, :, (c + 1) % C], other, die.at[0], die.at[1], to, q)
    swap.start()
    arrived(neg_y)
    neg = negp[q]
    for j in range(1, Y):
        neg = neg + negr[(q + j) % Y]
    neg_out[...] = neg
    loss = jnp.sum(neg) * (1.0 / BLK)
    edge = lax.broadcasted_iota(jnp.int32, (CAP, LANES), 1) < N
    count = jnp.sum(jnp.where(edge & (own[0] >= 0), 1.0, 0.0)) * BLK
    swap.wait_recv()
    v = part[:, :, c] + other[...]
    half[...] = v
    v = v * scale

    def back(k):
        to = ((z + k // X) % Z) * XC + ((x + k % X) % X) * C + c
        return copy(half.at[to // XC, (to % XC) // C], ret.at[z, x], back_s.at[k], back_r.at[k], to, q)

    def back_go(k, _):
        back(k).start()
        return 0

    def back_got(k, _):
        back(k).wait_recv()
        return 0

    lax.fori_loop(1, R, back_go, 0)
    lit = jnp.concatenate([ids[:, k * C + c][:, None] for k in range(X)], axis=1) >= 0
    lit = lit & (lax.broadcasted_iota(jnp.int32, (Z, X, RC, LANES), 3) < N)
    loss = loss + jnp.sum(jnp.where(lit, softplus(-v), 0.0))
    spot = lax.broadcasted_iota(jnp.int32, tot.shape[1:], 1)
    mine_sum = jnp.where(spot == 0, loss, jnp.where(spot == 1, count, 0.0))
    tot[0] = mine_sum
    ret[z, x] = half[z, x]

    add_c = start(c_stage(3, lambda to: tot.at[0], lc.at[xc]))
    lax.fori_loop(1, R, back_got, 0)
    arrived(add_c)
    total = mine_sum
    for k in range(1, XC):
        total = total + lc[behind(k) % XC]
    tot[1] = total
    add_z = start(z_stage(2, lambda to: tot.at[1], lz.at[z]))
    for k in range(R):
        at = pl.multiple_of((q * R + k) * RC, RC)
        tall[pl.ds(at, RC), :] = ret[k // X, k % X]
    for r in range(Y):
        for k in range(CAP):
            rows_b = tall[pl.ds(r * CAP + k, BLK, stride=RC), :]
            ysend[r, k] = jnp.swapaxes(rows_b, 0, 1)[:N]
    back_y = start(y_stage(2, lambda to: ysend.at[to], yrecv.at[q]))
    arrived(add_z)
    for j in range(1, Z):
        total = total + lz[(z + j) % Z]
    tot[2] = total
    add_y = start(y_stage(3, lambda to: tot.at[2], ly.at[q]))
    arrived(back_y)
    for k in range(CAP):
        v = ysend[q, k]
        for j in range(1, Y):
            v = v + yrecv[(q + j) % Y, k]
        pos_out[pl.ds(k, N, stride=CAP), :] = v
    arrived(add_y)
    for j in range(1, Y):
        total = total + ly[(q + j) % Y]
    loss_out[...] = total

    for copies in (ids_y, ids_z, ids_c, pool_z, pool_x, pool_c, neg_y, back_y, add_c, add_z, add_y):
        sent(copies)
    swap.wait_send()

    def bulk_sent(k, _):
        bulk(k).wait_send()
        return 0

    def back_sent(k, _):
        back(k).wait_send()
        return 0

    lax.fori_loop(1, N, bulk_sent, 0)
    lax.fori_loop(1, R, back_sent, 0)


def step(dims, features, w_in, w_out, pos_src, pos_dst, counts, neg_blocks, neg_pick):
    Z, X, C, Y = dims
    XC, N, R = X * C, Z * X * C, Z * X
    total, D = features.shape
    BLK = R * Y
    NB = total // BLK
    H = D // C
    CAP = pos_dst.shape[3]
    RC = Y * CAP
    NEG = neg_blocks.shape[1]
    bf, f32, i32 = jnp.bfloat16, jnp.float32, jnp.int32
    scale = 1.0 / D**0.5
    src, dst, pick = (t.reshape(N, CAP) for t in (pos_src, pos_dst, neg_pick))
    live = jnp.arange(CAP, dtype=i32)[None, :] < counts.reshape(N, 1)
    own = jnp.stack([jnp.where(live, src, -1), dst, pick, pick])
    own = jnp.transpose(own.reshape(2, 2, N, CAP), (0, 3, 1, 2))
    own = jnp.pad(own, ((0, 0), (0, 0), (0, 0), (0, HALF - N))).reshape(2, CAP, LANES)
    per, slots = (8, 4) if NB % 8 == 0 else (NB, 1)
    scratch = [
        pltpu.VMEM((NB, R, D), bf),
        pltpu.VMEM((slots, per, BLK, D), bf),
        pltpu.VMEM((NB, BLK, D), bf),
        pltpu.VMEM((R, C, NB, H), bf),
        pltpu.VMEM((N, NB, H), bf),
        pltpu.VMEM((Z, X, C, NEG, R, D), bf),
        pltpu.VMEM((Y, 2, RC, LANES), i32),
        pltpu.VMEM((Z, XC, RC, LANES), i32),
        pltpu.VMEM((N * RC, LANES), f32),
        pltpu.VMEM((2, RC, LANES), i32),
        pltpu.SMEM((2, RC, LANES), i32),
        pltpu.VMEM((N, 2, N * RC, H), bf),
        pltpu.VMEM((Z, X, C, RC, LANES), f32),
        pltpu.VMEM((Z, X, RC, LANES), f32),
        pltpu.VMEM((Z, X, RC, LANES), f32),
        pltpu.VMEM((Z, X, RC, LANES), f32),
        pltpu.VMEM((BLK * RC, LANES), f32),
        pltpu.VMEM((Y, CAP, N, BLK), f32),
        pltpu.VMEM((Y, CAP, N, BLK), f32),
        pltpu.VMEM((Y, N * CAP, BLK), f32),
        pltpu.VMEM((Y, N * CAP, BLK), f32),
        pltpu.VMEM((3, 8, LANES), f32),
        pltpu.VMEM((XC, 8, LANES), f32),
        pltpu.VMEM((Z, 8, LANES), f32),
        pltpu.VMEM((Y, 8, LANES), f32),
        DMA((N,)),
        DMA((N,)),
        DMA((R,)),
        DMA((R,)),
        DMA((4, Y)),
        DMA((4, Y)),
        DMA((4, XC)),
        DMA((4, XC)),
        DMA((3, Z)),
        DMA((3, Z)),
        DMA((2,)),
        DMA,
        DMA((slots,)),
    ]
    pos, neg, sums = pl.pallas_call(
        functools.partial(kernel, dims, scale),
        in_specs=[pl.BlockSpec(memory_space=pl.ANY), pl.BlockSpec(memory_space=pltpu.SMEM)] + [VMEM] * 3,
        out_specs=[VMEM] * 3,
        out_shape=[
            jax.ShapeDtypeStruct((N * CAP, BLK), f32),
            jax.ShapeDtypeStruct((N * CAP, BLK), f32),
            jax.ShapeDtypeStruct((8, LANES), f32),
        ],
        scratch_shapes=scratch,
        compiler_params=pltpu.CompilerParams(
            collective_id=0, has_side_effects=True, vmem_limit_bytes=60 * 2**20
        ),
        name="step",
    )(features.reshape(NB, BLK, D), neg_blocks, w_in, w_out, own)
    loss = sums[0, 0] / sums[0, 1]
    shape = (1, 1, N, CAP, BLK)
    return (pos * scale).reshape(shape), (neg * (1.0 / BLK)).reshape(shape), loss


def solution(mesh):
    n, reps = mesh.shape["node"], mesh.shape["rep"]
    dims = (n // 8, 4, 2, reps) if n >= 32 else (n // 4, 2, 2, reps)
    return jax.shard_map(
        functools.partial(step, dims),
        mesh=mesh,
        in_specs=(
            P("node", None),
            P(),
            P(),
            P("node", "rep", None, None),
            P("node", "rep", None, None),
            P("node", "rep", None),
            P("node", None),
            P("node", "rep", None, None),
        ),
        out_specs=(P("node", "rep", None, None, None), P("node", "rep", None, None, None), P()),
        check_vma=False,
    )
```

```python
import functools

import jax
import jax.numpy as jnp
from jax import lax
from jax.experimental import pallas as pl
from jax.experimental.pallas import tpu as pltpu
from jax.sharding import PartitionSpec as P

MESH = pl.DeviceIdType.MESH
VMEM = pl.BlockSpec(memory_space=pltpu.VMEM)
DMA = pltpu.SemaphoreType.DMA
LANES = 128
HALF = LANES // 2


def softplus(v):
    return jnp.maximum(v, 0.0) + jnp.log1p(jnp.exp(-jnp.abs(v)))


def bits(n):
    return n.bit_length() - 1


def kernel(
    dims, scale, feat, chosen, w_in, w_out, own, pos_out, neg_out, loss_out,
    xq, stage, emb, send, recv, pool, near, ids, idc, near_v, near_s, ends, part, other, half, ret, tall, ysend, yrecv,
    negp, negr, tot, lc, lz, ly,
    bulk_s, bulk_r, back_s, back_r, y_s, y_r, c_s, c_r, z_s, z_r, die, local, chunk_sem,
):
    Z, X, C, Y = dims
    XC, N = X * C, Z * X * C
    R = Z * X
    NB, BLK, D = emb.shape
    H = D // C
    CAP = ysend.shape[1]
    RC = Y * CAP
    NEG = pool.shape[3]
    me, q = lax.axis_index("node"), lax.axis_index("rep")
    z, xc = me // XC, me % XC
    x, c = xc // C, xc % C

    def ahead(k):
        dz, dx, dc = k // XC, (k // C) % X, k % C
        return ((z + dz) % Z) * XC + ((x + dx) % X) * C + (c + dc) % C

    def behind(k):
        dz, dx, dc = k // XC, (k // C) % X, k % C
        return ((z + Z - dz) % Z) * XC + ((x + X - dx) % X) * C + (c + C - dc) % C

    def copy(src, dst, s, r, node, rep):
        return pltpu.make_async_remote_copy(
            src_ref=src, dst_ref=dst, send_sem=s, recv_sem=r, device_id=(node, rep), device_id_type=MESH
        )

    def y_stage(n, src, dst):
        return [
            copy(src((q + j) % Y), dst, y_s.at[n, j], y_r.at[n, j], me, (q + j) % Y) for j in range(1, Y)
        ]

    def c_stage(n, src, dst):
        out = []
        for k in range(1, XC):
            to = ahead(k) % XC
            out.append(copy(src(to), dst, c_s.at[n, k], c_r.at[n, k], z * XC + to, q))
        return out

    def z_stage(n, src, dst):
        out = []
        for j in range(1, Z):
            to = (z + j) % Z
            out.append(copy(src(to), dst, z_s.at[n, j], z_r.at[n, j], to * XC + xc, q))
        return out

    def start(copies):
        for each in copies:
            each.start()
        return copies

    def arrived(copies):
        for each in copies:
            each.wait_recv()

    def sent(copies):
        for each in copies:
            each.wait_send()

    def encode(v):
        h = jnp.dot(v, w_in[...], preferred_element_type=jnp.float32)
        h = (0.5 * h * (1.0 + jnp.tanh(0.5 * h))).astype(jnp.bfloat16)
        return jnp.dot(h, w_out[...], preferred_element_type=jnp.float32).astype(jnp.bfloat16)

    barrier = pltpu.get_barrier_semaphore()

    def greet(k, _):
        pl.semaphore_signal(barrier, inc=1, device_id=(ahead(k), q), device_id_type=MESH)
        return 0

    lax.fori_loop(1, XC, greet, 0)
    for j in range(1, Z):
        to = ((z + j) % Z) * XC + xc
        pl.semaphore_signal(barrier, inc=1, device_id=(to, q), device_id_type=MESH)
    for j in range(1, Y):
        pl.semaphore_signal(barrier, inc=1, device_id=(me, (q + j) % Y), device_id_type=MESH)

    mine = pltpu.make_async_copy(feat.at[:, pl.ds(q * R, R), :], xq, local)
    mine.start()
    slots, per = stage.shape[0], stage.shape[1]
    chunks = NB // per

    def fetch(g, slot):
        return pltpu.make_async_copy(feat.at[pl.ds(g * per, per)], stage.at[slot], chunk_sem.at[slot])

    for g in range(min(slots, chunks)):
        fetch(g, g).start()

    tall[...] = jnp.zeros_like(tall)
    fill = lax.broadcasted_iota(jnp.int32, (2, RC, LANES), 1) // CAP == q
    near_v[...] = jnp.where(fill, jnp.concatenate([own[...]] * Y, axis=1), 0)
    mine.wait()
    offer = jnp.concatenate([xq[chosen[0, k]] for k in range(NEG)], axis=0)
    pool[z, x, c] = encode(offer).reshape(NEG, R, D)
    pl.semaphore_wait(barrier, XC + Z + Y - 3)
    ids_y = start(y_stage(0, lambda to: near_v, near.at[q]))
    pool_z = start(z_stage(0, lambda to: pool.at[z, x, c], pool.at[z, x, c]))

    G = 16 if NB % 16 == 0 else NB
    n = G * R
    i0 = lax.broadcasted_iota(jnp.int32, (n, n), 0)
    i1 = lax.broadcasted_iota(jnp.int32, (n, n), 1)
    perm = jnp.where(i1 == (i0 & (G - 1)) * R + (i0 >> bits(G)), 1.0, 0.0).astype(jnp.bfloat16)

    def rows(g, _):
        at = pl.multiple_of(g * G, G)
        e = encode(xq[pl.ds(at, G)].reshape(n, D))
        t = jnp.dot(perm, e, preferred_element_type=jnp.float32).astype(jnp.bfloat16)
        for k in range(C):
            send[:, k, pl.ds(at, G), :] = t[:, k * H : (k + 1) * H].reshape(R, G, H)
        return 0

    lax.fori_loop(0, NB // G, rows, 0)

    def bulk(k):
        to = ahead(k)
        return copy(send.at[to // C, to % C], recv.at[me], bulk_s.at[k], bulk_r.at[k], to, q)

    def column(m):
        return bulk((m // C) * XC + m % C)

    side = (X - 1) * C

    def others(m):
        return bulk((m // side) * XC + C + m % side)

    def column_go(m, _):
        column(m).start()
        return 0

    def others_go(m, _):
        others(m).start()
        return 0

    arrived(ids_y)
    tile = near_v[...]
    for j in range(1, Y):
        tile = tile + near[(q + j) % Y]
    near[q] = tile
    ids[z, xc] = tile[0]
    ids_z = start(z_stage(1, lambda to: ids.at[z, xc], ids.at[z, xc]))
    scalars = pltpu.make_async_copy(near.at[q], near_s, local)
    scalars.start()
    arrived(pool_z)
    pool_x = []
    for dx in range(1, X):
        to = z * XC + ((x + dx) % X) * C + c
        pool_x.append(copy(pool.at[:, x, c], pool.at[:, x, c], c_s.at[0, dx], c_r.at[0, dx], to, q))
    start(pool_x)
    lax.fori_loop(1, Z * C, column_go, 0)
    recv[me] = send[me // C, me % C]

    def full(g, _):
        slot = g % slots
        fetch(g, slot).wait()
        emb[pl.ds(g * per, per)] = encode(stage[slot].reshape(per * BLK, D)).reshape(per, BLK, D)

        @pl.when(g + slots < chunks)
        def _():
            fetch(g + slots, slot).start()

        return 0

    lax.fori_loop(0, chunks // 4, full, 0)
    arrived(ids_z)
    ids_c = start(c_stage(2, lambda to: ids.at[:, xc], ids.at[:, xc]))
    lax.fori_loop(chunks // 4, chunks, full, 0)
    arrived(pool_x)
    pool_c = []
    for dc in range(1, C):
        to = z * XC + x * C + (c + dc) % C
        pool_c.append(
            copy(pool.at[:, :, c], pool.at[:, :, c], c_s.at[1, dc], c_r.at[1, dc], to, q)
        )
    start(pool_c)
    lax.fori_loop(0, Z * side, others_go, 0)
    scalars.wait()
    arrived(pool_c)

    def negatives(e, _):
        for k in range(4 * CAP):
            r, o = e >> bits(N // 4), (e & (N // 4 - 1)) * 4 + k // CAP
            s = near_s[0, r * CAP + k % CAP, o]
            p = near_s[1, r * CAP + k % CAP, o]
            node = p >> bits(NEG)
            cand = pool[
                node >> bits(XC), (node >> bits(C)) & (X - 1), node & (C - 1), p & (NEG - 1)
            ]
            v = lax.dot_general(
                cand,
                emb[jnp.maximum(s, 0)],
                (((1,), (1,)), ((), ())),
                preferred_element_type=jnp.float32,
            )
            total = jnp.sum(softplus(v * scale), axis=0, keepdims=True)
            negp[r, pl.ds(o * CAP + k % CAP, 1), :] = jnp.where(s >= 0, total, 0.0)
        return 0

    lax.fori_loop(0, Y * N // 4, negatives, 0)
    neg_y = start(y_stage(1, lambda to: negp.at[to], negr.at[q]))

    arrived(ids_c)
    lane = lax.broadcasted_iota(jnp.int32, (N, LANES), 1)
    for k in range(RC):
        a = jnp.concatenate(
            [ids[i // XC, i % XC, pl.ds(k, 1), :].astype(jnp.float32) for i in range(N)], axis=0
        )
        t = jnp.swapaxes(jnp.concatenate([a] * (LANES // N), axis=0), 0, 1)[:N]
        idc[pl.ds(k, N, stride=RC), :] = jnp.where(lane < HALF, t, a)

    number = lax.broadcasted_iota(jnp.int32, (N * RC, LANES), 1).astype(jnp.float32)

    def gather(s):
        hots = []
        for k in range(2):
            at = jnp.full((N * RC, LANES), s + k * HALF, jnp.int32)
            col = jnp.take_along_axis(idc[...], at, axis=1)
            hot = [jnp.where(col == number, 1.0, 0.0).astype(jnp.bfloat16)]
            if NB > LANES:
                rest = jnp.where(col == number + LANES, 1.0, 0.0).astype(jnp.bfloat16)
                hot.append(rest[:, : NB - LANES])
            hots.append(jnp.concatenate(hot, axis=1)[:, :NB])
        hot = jnp.concatenate(hots, axis=0)
        got = jnp.dot(hot, recv[s], preferred_element_type=jnp.float32).astype(jnp.bfloat16)
        ends[s] = got.reshape(2, N * RC, H)

    def node_column(m):
        return behind((m // C) * XC + m % C)

    def node_others(m):
        return behind((m // side) * XC + C + m % side)

    def gather_column(m, _):
        for k in range(2):
            column(2 * m + k).wait_recv()
        for k in range(2):
            gather(node_column(2 * m + k))
        return 0

    def gather_others(m, _):
        for k in range(2):
            others(2 * m + k).wait_recv()
        for k in range(2):
            gather(node_others(2 * m + k))
        return 0

    column(1).wait_recv()
    gather(me)
    gather(node_column(1))
    lax.fori_loop(1, Z * C // 2, gather_column, 0)
    lax.fori_loop(0, Z * side // 2, gather_others, 0)

    shape = (N, RC, LANES)
    keep = lax.broadcasted_iota(jnp.int32, shape, 0) == lax.broadcasted_iota(jnp.int32, shape, 2)

    def dots(h, _):
        at = pl.multiple_of(h * 4 * RC, 4 * RC)
        b = ends[:, 1, pl.ds(at, 4 * RC), :].astype(jnp.float32)
        for k in range(4):
            i = 4 * h + k
            a = ends[i, 0].astype(jnp.float32).reshape(N, RC, H)
            sums = jnp.sum(a * b[:, k * RC : (k + 1) * RC], axis=2, keepdims=True)
            part[i // XC, (i % XC) // C, i % C] = jnp.sum(jnp.where(keep, sums, 0.0), axis=0)
        return 0

    lax.fori_loop(0, N // 4, dots, 0)

    to = z * XC + x * C + (c + 1) % C
    swap = copy(part.at[:, :, (c + 1) % C], other, die.at[0], die.at[1], to, q)
    swap.start()
    arrived(neg_y)
    neg = negp[q]
    for j in range(1, Y):
        neg = neg + negr[(q + j) % Y]
    neg_out[...] = neg
    loss = jnp.sum(neg) * (1.0 / BLK)
    edge = lax.broadcasted_iota(jnp.int32, (CAP, LANES), 1) < N
    count = jnp.sum(jnp.where(edge & (own[0] >= 0), 1.0, 0.0)) * BLK
    swap.wait_recv()
    v = part[:, :, c] + other[...]
    half[...] = v
    v = v * scale

    def back(k):
        to = ((z + k // X) % Z) * XC + ((x + k % X) % X) * C + c
        return copy(half.at[to // XC, (to % XC) // C], ret.at[z, x], back_s.at[k], back_r.at[k], to, q)

    def back_go(k, _):
        back(k).start()
        return 0

    def back_got(k, _):
        back(k).wait_recv()
        return 0

    lax.fori_loop(1, R, back_go, 0)
    lit = jnp.concatenate([ids[:, k * C + c][:, None] for k in range(X)], axis=1) >= 0
    lit = lit & (lax.broadcasted_iota(jnp.int32, (Z, X, RC, LANES), 3) < N)
    loss = loss + jnp.sum(jnp.where(lit, softplus(-v), 0.0))
    spot = lax.broadcasted_iota(jnp.int32, tot.shape[1:], 1)
    mine_sum = jnp.where(spot == 0, loss, jnp.where(spot == 1, count, 0.0))
    tot[0] = mine_sum
    ret[z, x] = half[z, x]

    add_c = start(c_stage(3, lambda to: tot.at[0], lc.at[xc]))
    lax.fori_loop(1, R, back_got, 0)
    arrived(add_c)
    total = mine_sum
    for k in range(1, XC):
        total = total + lc[behind(k) % XC]
    tot[1] = total
    add_z = start(z_stage(2, lambda to: tot.at[1], lz.at[z]))
    for k in range(R):
        at = pl.multiple_of((q * R + k) * RC, RC)
        tall[pl.ds(at, RC), :] = ret[k // X, k % X]
    for r in range(Y):
        for k in range(CAP):
            rows_b = tall[pl.ds(r * CAP + k, BLK, stride=RC), :]
            ysend[r, k] = jnp.swapaxes(rows_b, 0, 1)[:N]
    back_y = start(y_stage(2, lambda to: ysend.at[to], yrecv.at[q]))
    arrived(add_z)
    for j in range(1, Z):
        total = total + lz[(z + j) % Z]
    tot[2] = total
    add_y = start(y_stage(3, lambda to: tot.at[2], ly.at[q]))
    arrived(back_y)
    for k in range(CAP):
        v = ysend[q, k]
        for j in range(1, Y):
            v = v + yrecv[(q + j) % Y, k]
        pos_out[pl.ds(k, N, stride=CAP), :] = v
    arrived(add_y)
    for j in range(1, Y):
        total = total + ly[(q + j) % Y]
    loss_out[...] = total

    for copies in (ids_y, ids_z, ids_c, pool_z, pool_x, pool_c, neg_y, back_y, add_c, add_z, add_y):
        sent(copies)
    swap.wait_send()

    def bulk_sent(k, _):
        bulk(k).wait_send()
        return 0

    def back_sent(k, _):
        back(k).wait_send()
        return 0

    lax.fori_loop(1, N, bulk_sent, 0)
    lax.fori_loop(1, R, back_sent, 0)


def step(dims, features, w_in, w_out, pos_src, pos_dst, counts, neg_blocks, neg_pick):
    Z, X, C, Y = dims
    XC, N, R = X * C, Z * X * C, Z * X
    total, D = features.shape
    BLK = R * Y
    NB = total // BLK
    H = D // C
    CAP = pos_dst.shape[3]
    RC = Y * CAP
    NEG = neg_blocks.shape[1]
    bf, f32, i32 = jnp.bfloat16, jnp.float32, jnp.int32
    scale = 1.0 / D**0.5
    src, dst, pick = (t.reshape(N, CAP) for t in (pos_src, pos_dst, neg_pick))
    live = jnp.arange(CAP, dtype=i32)[None, :] < counts.reshape(N, 1)
    own = jnp.stack([jnp.where(live, src, -1), dst, pick, pick])
    own = jnp.transpose(own.reshape(2, 2, N, CAP), (0, 3, 1, 2))
    own = jnp.pad(own, ((0, 0), (0, 0), (0, 0), (0, HALF - N))).reshape(2, CAP, LANES)
    per, slots = (8, 4) if NB % 8 == 0 else (NB, 1)
    scratch = [
        pltpu.VMEM((NB, R, D), bf),
        pltpu.VMEM((slots, per, BLK, D), bf),
        pltpu.VMEM((NB, BLK, D), bf),
        pltpu.VMEM((R, C, NB, H), bf),
        pltpu.VMEM((N, NB, H), bf),
        pltpu.VMEM((Z, X, C, NEG, R, D), bf),
        pltpu.VMEM((Y, 2, RC, LANES), i32),
        pltpu.VMEM((Z, XC, RC, LANES), i32),
        pltpu.VMEM((N * RC, LANES), f32),
        pltpu.VMEM((2, RC, LANES), i32),
        pltpu.SMEM((2, RC, LANES), i32),
        pltpu.VMEM((N, 2, N * RC, H), bf),
        pltpu.VMEM((Z, X, C, RC, LANES), f32),
        pltpu.VMEM((Z, X, RC, LANES), f32),
        pltpu.VMEM((Z, X, RC, LANES), f32),
        pltpu.VMEM((Z, X, RC, LANES), f32),
        pltpu.VMEM((BLK * RC, LANES), f32),
        pltpu.VMEM((Y, CAP, N, BLK), f32),
        pltpu.VMEM((Y, CAP, N, BLK), f32),
        pltpu.VMEM((Y, N * CAP, BLK), f32),
        pltpu.VMEM((Y, N * CAP, BLK), f32),
        pltpu.VMEM((3, 8, LANES), f32),
        pltpu.VMEM((XC, 8, LANES), f32),
        pltpu.VMEM((Z, 8, LANES), f32),
        pltpu.VMEM((Y, 8, LANES), f32),
        DMA((N,)),
        DMA((N,)),
        DMA((R,)),
        DMA((R,)),
        DMA((4, Y)),
        DMA((4, Y)),
        DMA((4, XC)),
        DMA((4, XC)),
        DMA((3, Z)),
        DMA((3, Z)),
        DMA((2,)),
        DMA,
        DMA((slots,)),
    ]
    pos, neg, sums = pl.pallas_call(
        functools.partial(kernel, dims, scale),
        in_specs=[pl.BlockSpec(memory_space=pl.ANY), pl.BlockSpec(memory_space=pltpu.SMEM)] + [VMEM] * 3,
        out_specs=[VMEM] * 3,
        out_shape=[
            jax.ShapeDtypeStruct((N * CAP, BLK), f32),
            jax.ShapeDtypeStruct((N * CAP, BLK), f32),
            jax.ShapeDtypeStruct((8, LANES), f32),
        ],
        scratch_shapes=scratch,
        compiler_params=pltpu.CompilerParams(
            collective_id=0, has_side_effects=True, vmem_limit_bytes=60 * 2**20
        ),
        name="step",
    )(features.reshape(NB, BLK, D), neg_blocks, w_in, w_out, own)
    loss = sums[0, 0] / sums[0, 1]
    shape = (1, 1, N, CAP, BLK)
    return (pos * scale).reshape(shape), (neg * (1.0 / BLK)).reshape(shape), loss


def solution(mesh):
    n, reps = mesh.shape["node"], mesh.shape["rep"]
    dims = (n // 8, 4, 2, reps) if n >= 32 else (n // 4, 2, 2, reps)
    return jax.shard_map(
        functools.partial(step, dims),
        mesh=mesh,
        in_specs=(
            P("node", None),
            P(),
            P(),
            P("node", "rep", None, None),
            P("node", "rep", None, None),
            P("node", "rep", None),
            P("node", None),
            P("node", "rep", None, None),
        ),
        out_specs=(P("node", "rep", None, None, None), P("node", "rep", None, None, None), P()),
        check_vma=False,
    )
```

```python
import functools

import jax
import jax.numpy as jnp
from jax import lax
from jax.experimental import pallas as pl
from jax.experimental.pallas import tpu as pltpu
from jax.sharding import PartitionSpec as P

MESH = pl.DeviceIdType.MESH
VMEM = pl.BlockSpec(memory_space=pltpu.VMEM)
DMA = pltpu.SemaphoreType.DMA
LANES = 128
HALF = LANES // 2


def softplus(v):
    return jnp.maximum(v, 0.0) + jnp.log1p(jnp.exp(-jnp.abs(v)))


def bits(n):
    return n.bit_length() - 1


def kernel(
    dims, scale, feat, chosen, w_in, w_out, src, dst, picked, counts, pos_out, neg_out, loss_out,
    xq, stage, emb, send, recv, pool, near, ids, idc, near_v, near_s, ends, part, other, half, ret, tall, ysend, yrecv,
    negp, negr, tot, lc, lz, ly,
    bulk_s, bulk_r, back_s, back_r, y_s, y_r, c_s, c_r, z_s, z_r, die, local, chunk_sem,
):
    Z, X, C, Y = dims
    XC, N = X * C, Z * X * C
    R = Z * X
    NB, BLK, D = emb.shape
    H = D // C
    CAP = ysend.shape[1]
    RC = Y * CAP
    NEG = pool.shape[3]
    me, q = lax.axis_index("node"), lax.axis_index("rep")
    z, xc = me // XC, me % XC
    x, c = xc // C, xc % C

    def ahead(k):
        dz, dx, dc = k // XC, (k // C) % X, k % C
        return ((z + dz) % Z) * XC + ((x + dx) % X) * C + (c + dc) % C

    def behind(k):
        dz, dx, dc = k // XC, (k // C) % X, k % C
        return ((z + Z - dz) % Z) * XC + ((x + X - dx) % X) * C + (c + C - dc) % C

    def copy(src, dst, s, r, node, rep):
        return pltpu.make_async_remote_copy(
            src_ref=src, dst_ref=dst, send_sem=s, recv_sem=r, device_id=(node, rep), device_id_type=MESH
        )

    def y_stage(n, src, dst):
        return [
            copy(src((q + j) % Y), dst, y_s.at[n, j], y_r.at[n, j], me, (q + j) % Y) for j in range(1, Y)
        ]

    def c_stage(n, src, dst):
        out = []
        for k in range(1, XC):
            to = ahead(k) % XC
            out.append(copy(src(to), dst, c_s.at[n, k], c_r.at[n, k], z * XC + to, q))
        return out

    def z_stage(n, src, dst):
        out = []
        for j in range(1, Z):
            to = (z + j) % Z
            out.append(copy(src(to), dst, z_s.at[n, j], z_r.at[n, j], to * XC + xc, q))
        return out

    def start(copies):
        for each in copies:
            each.start()
        return copies

    def arrived(copies):
        for each in copies:
            each.wait_recv()

    def sent(copies):
        for each in copies:
            each.wait_send()

    def encode(v):
        h = jnp.dot(v, w_in[...], preferred_element_type=jnp.float32)
        h = (0.5 * h * (1.0 + jnp.tanh(0.5 * h))).astype(jnp.bfloat16)
        return jnp.dot(h, w_out[...], preferred_element_type=jnp.float32).astype(jnp.bfloat16)

    barrier = pltpu.get_barrier_semaphore()

    def greet(k, _):
        pl.semaphore_signal(barrier, inc=1, device_id=(ahead(k), q), device_id_type=MESH)
        return 0

    lax.fori_loop(1, XC, greet, 0)
    for j in range(1, Z):
        to = ((z + j) % Z) * XC + xc
        pl.semaphore_signal(barrier, inc=1, device_id=(to, q), device_id_type=MESH)
    for j in range(1, Y):
        pl.semaphore_signal(barrier, inc=1, device_id=(me, (q + j) % Y), device_id_type=MESH)

    mine = pltpu.make_async_copy(feat.at[:, pl.ds(q * R, R), :], xq, local)
    mine.start()
    slots, per = stage.shape[0], stage.shape[1]
    chunks = NB // per

    def fetch(g, slot):
        return pltpu.make_async_copy(feat.at[pl.ds(g * per, per)], stage.at[slot], chunk_sem.at[slot])

    for g in range(min(slots, chunks)):
        fetch(g, g).start()

    tall[...] = jnp.zeros_like(tall)
    fill = lax.broadcasted_iota(jnp.int32, (2, RC, LANES), 1) // CAP == q
    alive = lax.broadcasted_iota(jnp.int32, (CAP, N), 0) < counts[...]

    def pair(a, b):
        gap = [] if N == HALF else [jnp.zeros((CAP, HALF - N), jnp.int32)]
        return jnp.concatenate([a] + gap + [b] + gap, axis=1)

    own = jnp.stack([pair(jnp.where(alive, src[...], -1), dst[...]), pair(picked[...], picked[...])])
    near_v[...] = jnp.where(fill, jnp.concatenate([own] * Y, axis=1), 0)
    mine.wait()
    offer = jnp.concatenate([xq[chosen[0, k]] for k in range(NEG)], axis=0)
    pool[z, x, c] = encode(offer).reshape(NEG, R, D)
    pl.semaphore_wait(barrier, XC + Z + Y - 3)
    ids_y = start(y_stage(0, lambda to: near_v, near.at[q]))
    pool_z = start(z_stage(0, lambda to: pool.at[z, x, c], pool.at[z, x, c]))

    G = 16 if NB % 16 == 0 else NB
    n = G * R
    i0 = lax.broadcasted_iota(jnp.int32, (n, n), 0)
    i1 = lax.broadcasted_iota(jnp.int32, (n, n), 1)
    perm = jnp.where(i1 == (i0 & (G - 1)) * R + (i0 >> bits(G)), 1.0, 0.0).astype(jnp.bfloat16)

    def rows(g, _):
        at = pl.multiple_of(g * G, G)
        e = encode(xq[pl.ds(at, G)].reshape(n, D))
        t = jnp.dot(perm, e, preferred_element_type=jnp.float32).astype(jnp.bfloat16)
        for k in range(C):
            send[:, k, pl.ds(at, G), :] = t[:, k * H : (k + 1) * H].reshape(R, G, H)
        return 0

    lax.fori_loop(0, NB // G, rows, 0)

    def bulk(k):
        to = ahead(k)
        return copy(send.at[to // C, to % C], recv.at[me], bulk_s.at[k], bulk_r.at[k], to, q)

    def turn(i):
        return jnp.where(i % 2 == 1, (i + 1) // 2, (Z - i // 2) % Z)

    def column(m):
        return bulk(turn(m // C) * XC + m % C)

    side = (X - 1) * C

    def others(m):
        return bulk(turn(m // side) * XC + C + m % side)

    def column_go(m, _):
        column(m).start()
        return 0

    def others_go(m, _):
        others(m).start()
        return 0

    arrived(ids_y)
    tile = near_v[...]
    for j in range(1, Y):
        tile = tile + near[(q + j) % Y]
    near[q] = tile
    ids[z, xc] = tile[0]
    ids_z = start(z_stage(1, lambda to: ids.at[z, xc], ids.at[z, xc]))
    scalars = pltpu.make_async_copy(near.at[q], near_s, local)
    scalars.start()
    arrived(pool_z)
    pool_x = []
    for dx in range(1, X):
        to = z * XC + ((x + dx) % X) * C + c
        pool_x.append(copy(pool.at[:, x, c], pool.at[:, x, c], c_s.at[0, dx], c_r.at[0, dx], to, q))
    start(pool_x)
    lax.fori_loop(1, Z * C, column_go, 0)
    recv[me] = send[me // C, me % C]

    def full(g, _):
        slot = g % slots
        fetch(g, slot).wait()
        emb[pl.ds(g * per, per)] = encode(stage[slot].reshape(per * BLK, D)).reshape(per, BLK, D)

        @pl.when(g + slots < chunks)
        def _():
            fetch(g + slots, slot).start()

        return 0

    lax.fori_loop(0, chunks // 4, full, 0)
    arrived(ids_z)
    ids_c = start(c_stage(2, lambda to: ids.at[:, xc], ids.at[:, xc]))
    lax.fori_loop(chunks // 4, chunks, full, 0)
    arrived(pool_x)
    pool_c = []
    for dc in range(1, C):
        to = z * XC + x * C + (c + dc) % C
        pool_c.append(
            copy(pool.at[:, :, c], pool.at[:, :, c], c_s.at[1, dc], c_r.at[1, dc], to, q)
        )
    start(pool_c)
    lax.fori_loop(0, Z * side, others_go, 0)
    scalars.wait()
    arrived(pool_c)

    def negatives(e, _):
        for k in range(4 * CAP):
            r, o = e >> bits(N // 4), (e & (N // 4 - 1)) * 4 + k // CAP
            s = near_s[0, r * CAP + k % CAP, o]
            p = near_s[1, r * CAP + k % CAP, o]
            node = p >> bits(NEG)
            cand = pool[
                node >> bits(XC), (node >> bits(C)) & (X - 1), node & (C - 1), p & (NEG - 1)
            ]
            v = lax.dot_general(
                cand,
                emb[jnp.maximum(s, 0)],
                (((1,), (1,)), ((), ())),
                preferred_element_type=jnp.float32,
            )
            total = jnp.sum(softplus(v * scale), axis=0, keepdims=True)
            negp[r, pl.ds(o * CAP + k % CAP, 1), :] = jnp.where(s >= 0, total, 0.0)
        return 0

    lax.fori_loop(0, Y * N // 4, negatives, 0)
    neg_y = start(y_stage(1, lambda to: negp.at[to], negr.at[q]))

    arrived(ids_c)
    lane = lax.broadcasted_iota(jnp.int32, (N, LANES), 1)
    for k in range(RC):
        a = jnp.concatenate(
            [ids[i // XC, i % XC, pl.ds(k, 1), :].astype(jnp.float32) for i in range(N)], axis=0
        )
        t = jnp.swapaxes(jnp.concatenate([a] * (LANES // N), axis=0), 0, 1)[:N]
        idc[pl.ds(k, N, stride=RC), :] = jnp.where(lane < HALF, t, a)

    number = lax.broadcasted_iota(jnp.int32, (N * RC, LANES), 1).astype(jnp.float32)

    def gather(s):
        hots = []
        for k in range(2):
            at = jnp.full((N * RC, LANES), s + k * HALF, jnp.int32)
            col = jnp.take_along_axis(idc[...], at, axis=1)
            hot = [jnp.where(col == number, 1.0, 0.0).astype(jnp.bfloat16)]
            if NB > LANES:
                rest = jnp.where(col == number + LANES, 1.0, 0.0).astype(jnp.bfloat16)
                hot.append(rest[:, : NB - LANES])
            hots.append(jnp.concatenate(hot, axis=1)[:, :NB])
        hot = jnp.concatenate(hots, axis=0)
        got = jnp.dot(hot, recv[s], preferred_element_type=jnp.float32).astype(jnp.bfloat16)
        ends[s] = got.reshape(2, N * RC, H)

    def node_column(m):
        return behind(turn(m // C) * XC + m % C)

    def node_others(m):
        return behind(turn(m // side) * XC + C + m % side)

    def gather_column(m, _):
        for k in range(2):
            column(2 * m + k).wait_recv()
        for k in range(2):
            gather(node_column(2 * m + k))
        return 0

    def gather_others(m, _):
        for k in range(2):
            others(2 * m + k).wait_recv()
        for k in range(2):
            gather(node_others(2 * m + k))
        return 0

    column(1).wait_recv()
    gather(me)
    gather(node_column(1))
    lax.fori_loop(1, Z * C // 2, gather_column, 0)
    lax.fori_loop(0, Z * side // 2, gather_others, 0)

    shape = (N, RC, LANES)
    keep = lax.broadcasted_iota(jnp.int32, shape, 0) == lax.broadcasted_iota(jnp.int32, shape, 2)

    def dots(h, _):
        at = pl.multiple_of(h * 4 * RC, 4 * RC)
        b = ends[:, 1, pl.ds(at, 4 * RC), :].astype(jnp.float32)
        for k in range(4):
            i = 4 * h + k
            a = ends[i, 0].astype(jnp.float32).reshape(N, RC, H)
            sums = jnp.sum(a * b[:, k * RC : (k + 1) * RC], axis=2, keepdims=True)
            part[i // XC, (i % XC) // C, i % C] = jnp.sum(jnp.where(keep, sums, 0.0), axis=0)
        return 0

    lax.fori_loop(0, N // 4, dots, 0)

    to = z * XC + x * C + (c + 1) % C
    swap = copy(part.at[:, :, (c + 1) % C], other, die.at[0], die.at[1], to, q)
    swap.start()
    arrived(neg_y)
    neg = negp[q]
    for j in range(1, Y):
        neg = neg + negr[(q + j) % Y]
    neg_out[...] = neg
    loss = jnp.sum(neg) * (1.0 / BLK)
    count = jnp.sum(jnp.where(alive, 1.0, 0.0)) * BLK
    swap.wait_recv()
    v = part[:, :, c] + other[...]
    half[...] = v
    v = v * scale

    def back(k):
        to = ((z + k // X) % Z) * XC + ((x + k % X) % X) * C + c
        return copy(half.at[to // XC, (to % XC) // C], ret.at[z, x], back_s.at[k], back_r.at[k], to, q)

    def back_go(k, _):
        back(k).start()
        return 0

    def back_got(k, _):
        back(k).wait_recv()
        return 0

    lax.fori_loop(1, R, back_go, 0)
    lit = jnp.concatenate([ids[:, k * C + c][:, None] for k in range(X)], axis=1) >= 0
    lit = lit & (lax.broadcasted_iota(jnp.int32, (Z, X, RC, LANES), 3) < N)
    loss = loss + jnp.sum(jnp.where(lit, softplus(-v), 0.0))
    spot = lax.broadcasted_iota(jnp.int32, tot.shape[1:], 1)
    mine_sum = jnp.where(spot == 0, loss, jnp.where(spot == 1, count, 0.0))
    tot[0] = mine_sum
    ret[z, x] = half[z, x]

    add_c = start(c_stage(3, lambda to: tot.at[0], lc.at[xc]))
    lax.fori_loop(1, R, back_got, 0)
    arrived(add_c)
    total = mine_sum
    for k in range(1, XC):
        total = total + lc[behind(k) % XC]
    tot[1] = total
    add_z = start(z_stage(2, lambda to: tot.at[1], lz.at[z]))
    for k in range(R):
        at = pl.multiple_of((q * R + k) * RC, RC)
        tall[pl.ds(at, RC), :] = ret[k // X, k % X]
    for r in range(Y):
        for k in range(CAP):
            rows_b = tall[pl.ds(r * CAP + k, BLK, stride=RC), :]
            ysend[r, k] = jnp.swapaxes(rows_b, 0, 1)[:N]
    back_y = start(y_stage(2, lambda to: ysend.at[to], yrecv.at[q]))
    arrived(add_z)
    for j in range(1, Z):
        total = total + lz[(z + j) % Z]
    tot[2] = total
    add_y = start(y_stage(3, lambda to: tot.at[2], ly.at[q]))
    arrived(back_y)
    for k in range(CAP):
        v = ysend[q, k]
        for j in range(1, Y):
            v = v + yrecv[(q + j) % Y, k]
        pos_out[pl.ds(k, N, stride=CAP), :] = v
    arrived(add_y)
    for j in range(1, Y):
        total = total + ly[(q + j) % Y]
    loss_out[...] = total

    for copies in (ids_y, ids_z, ids_c, pool_z, pool_x, pool_c, neg_y, back_y, add_c, add_z, add_y):
        sent(copies)
    swap.wait_send()

    def bulk_sent(k, _):
        bulk(k).wait_send()
        return 0

    def back_sent(k, _):
        back(k).wait_send()
        return 0

    lax.fori_loop(1, N, bulk_sent, 0)
    lax.fori_loop(1, R, back_sent, 0)


def step(dims, features, w_in, w_out, pos_src, pos_dst, counts, neg_blocks, neg_pick):
    Z, X, C, Y = dims
    XC, N, R = X * C, Z * X * C, Z * X
    total, D = features.shape
    BLK = R * Y
    NB = total // BLK
    H = D // C
    CAP = pos_dst.shape[3]
    RC = Y * CAP
    NEG = neg_blocks.shape[1]
    bf, f32, i32 = jnp.bfloat16, jnp.float32, jnp.int32
    scale = 1.0 / D**0.5
    src, dst, pick = (t.reshape(N, CAP).T for t in (pos_src, pos_dst, neg_pick))
    per, slots = (8, 4) if NB % 8 == 0 else (NB, 1)
    scratch = [
        pltpu.VMEM((NB, R, D), bf),
        pltpu.VMEM((slots, per, BLK, D), bf),
        pltpu.VMEM((NB, BLK, D), bf),
        pltpu.VMEM((R, C, NB, H), bf),
        pltpu.VMEM((N, NB, H), bf),
        pltpu.VMEM((Z, X, C, NEG, R, D), bf),
        pltpu.VMEM((Y, 2, RC, LANES), i32),
        pltpu.VMEM((Z, XC, RC, LANES), i32),
        pltpu.VMEM((N * RC, LANES), f32),
        pltpu.VMEM((2, RC, LANES), i32),
        pltpu.SMEM((2, RC, LANES), i32),
        pltpu.VMEM((N, 2, N * RC, H), bf),
        pltpu.VMEM((Z, X, C, RC, LANES), f32),
        pltpu.VMEM((Z, X, RC, LANES), f32),
        pltpu.VMEM((Z, X, RC, LANES), f32),
        pltpu.VMEM((Z, X, RC, LANES), f32),
        pltpu.VMEM((BLK * RC, LANES), f32),
        pltpu.VMEM((Y, CAP, N, BLK), f32),
        pltpu.VMEM((Y, CAP, N, BLK), f32),
        pltpu.VMEM((Y, N * CAP, BLK), f32),
        pltpu.VMEM((Y, N * CAP, BLK), f32),
        pltpu.VMEM((3, 8, LANES), f32),
        pltpu.VMEM((XC, 8, LANES), f32),
        pltpu.VMEM((Z, 8, LANES), f32),
        pltpu.VMEM((Y, 8, LANES), f32),
        DMA((N,)),
        DMA((N,)),
        DMA((R,)),
        DMA((R,)),
        DMA((4, Y)),
        DMA((4, Y)),
        DMA((4, XC)),
        DMA((4, XC)),
        DMA((3, Z)),
        DMA((3, Z)),
        DMA((2,)),
        DMA,
        DMA((slots,)),
    ]
    pos, neg, sums = pl.pallas_call(
        functools.partial(kernel, dims, scale),
        in_specs=[pl.BlockSpec(memory_space=pl.ANY), pl.BlockSpec(memory_space=pltpu.SMEM)] + [VMEM] * 6,
        out_specs=[VMEM] * 3,
        out_shape=[
            jax.ShapeDtypeStruct((N * CAP, BLK), f32),
            jax.ShapeDtypeStruct((N * CAP, BLK), f32),
            jax.ShapeDtypeStruct((8, LANES), f32),
        ],
        scratch_shapes=scratch,
        compiler_params=pltpu.CompilerParams(
            collective_id=0, has_side_effects=True, vmem_limit_bytes=60 * 2**20
        ),
        name="step",
    )(features.reshape(NB, BLK, D), neg_blocks, w_in, w_out, src, dst, pick, counts.reshape(1, N))
    loss = sums[0, 0] / sums[0, 1]
    shape = (1, 1, N, CAP, BLK)
    return (pos * scale).reshape(shape), (neg * (1.0 / BLK)).reshape(shape), loss


def solution(mesh):
    n, reps = mesh.shape["node"], mesh.shape["rep"]
    dims = (n // 8, 4, 2, reps) if n >= 32 else (n // 4, 2, 2, reps)
    return jax.shard_map(
        functools.partial(step, dims),
        mesh=mesh,
        in_specs=(
            P("node", None),
            P(),
            P(),
            P("node", "rep", None, None),
            P("node", "rep", None, None),
            P("node", "rep", None),
            P("node", None),
            P("node", "rep", None, None),
        ),
        out_specs=(P("node", "rep", None, None, None), P("node", "rep", None, None, None), P()),
        check_vma=False,
    )
```

```python
import functools

import jax
import jax.numpy as jnp
from jax import lax
from jax.experimental import pallas as pl
from jax.experimental.pallas import tpu as pltpu
from jax.sharding import PartitionSpec as P

MESH = pl.DeviceIdType.MESH
VMEM = pl.BlockSpec(memory_space=pltpu.VMEM)
DMA = pltpu.SemaphoreType.DMA
LANES = 128
HALF = LANES // 2


def softplus(v):
    return jnp.maximum(v, 0.0) + jnp.log1p(jnp.exp(-jnp.abs(v)))


def bits(n):
    return n.bit_length() - 1


def kernel(
    dims, scale, feat, chosen, w_in, w_out, src, dst, picked, counts, pos_out, neg_out, loss_out,
    xq, stage, emb, send, recv, pool, near, ids, idc, near_v, near_s, ends, part, other, half, ret, tall, ysend, yrecv,
    negp, negr, tot, lc, lz, ly,
    bulk_s, bulk_r, back_s, back_r, y_s, y_r, c_s, c_r, z_s, z_r, die, local, chunk_sem,
):
    Z, X, C, Y = dims
    XC, N = X * C, Z * X * C
    R = Z * X
    NB, BLK, D = emb.shape
    H = D // C
    CAP = ysend.shape[1]
    RC = Y * CAP
    NEG = pool.shape[3]
    me, q = lax.axis_index("node"), lax.axis_index("rep")
    z, xc = me // XC, me % XC
    x, c = xc // C, xc % C

    def ahead(k):
        dz, dx, dc = k // XC, (k // C) % X, k % C
        return ((z + dz) % Z) * XC + ((x + dx) % X) * C + (c + dc) % C

    def behind(k):
        dz, dx, dc = k // XC, (k // C) % X, k % C
        return ((z + Z - dz) % Z) * XC + ((x + X - dx) % X) * C + (c + C - dc) % C

    def copy(src, dst, s, r, node, rep):
        return pltpu.make_async_remote_copy(
            src_ref=src, dst_ref=dst, send_sem=s, recv_sem=r, device_id=(node, rep), device_id_type=MESH
        )

    def y_stage(n, src, dst):
        return [
            copy(src((q + j) % Y), dst, y_s.at[n, j], y_r.at[n, j], me, (q + j) % Y) for j in range(1, Y)
        ]

    def c_stage(n, src, dst):
        out = []
        for k in range(1, XC):
            to = ahead(k) % XC
            out.append(copy(src(to), dst, c_s.at[n, k], c_r.at[n, k], z * XC + to, q))
        return out

    def z_stage(n, src, dst):
        out = []
        for j in range(1, Z):
            to = (z + j) % Z
            out.append(copy(src(to), dst, z_s.at[n, j], z_r.at[n, j], to * XC + xc, q))
        return out

    def start(copies):
        for each in copies:
            each.start()
        return copies

    def arrived(copies):
        for each in copies:
            each.wait_recv()

    def sent(copies):
        for each in copies:
            each.wait_send()

    def encode(v):
        h = jnp.dot(v, w_in[...], preferred_element_type=jnp.float32)
        h = (0.5 * h * (1.0 + jnp.tanh(0.5 * h))).astype(jnp.bfloat16)
        return jnp.dot(h, w_out[...], preferred_element_type=jnp.float32).astype(jnp.bfloat16)

    barrier = pltpu.get_barrier_semaphore()

    def greet(k, _):
        pl.semaphore_signal(barrier, inc=1, device_id=(ahead(k), q), device_id_type=MESH)
        return 0

    lax.fori_loop(1, XC, greet, 0)
    for j in range(1, Z):
        to = ((z + j) % Z) * XC + xc
        pl.semaphore_signal(barrier, inc=1, device_id=(to, q), device_id_type=MESH)
    for j in range(1, Y):
        pl.semaphore_signal(barrier, inc=1, device_id=(me, (q + j) % Y), device_id_type=MESH)

    mine = pltpu.make_async_copy(feat.at[:, pl.ds(q * R, R), :], xq, local)
    mine.start()
    slots, per = stage.shape[0], stage.shape[1]
    chunks = NB // per

    def fetch(g, slot):
        return pltpu.make_async_copy(feat.at[pl.ds(g * per, per)], stage.at[slot], chunk_sem.at[slot])

    for g in range(min(slots, chunks)):
        fetch(g, g).start()

    tall[...] = jnp.zeros_like(tall)
    fill = lax.broadcasted_iota(jnp.int32, (2, RC, LANES), 1) // CAP == q
    alive = lax.broadcasted_iota(jnp.int32, (CAP, N), 0) < counts[...]

    def pair(a, b):
        gap = [] if N == HALF else [jnp.zeros((CAP, HALF - N), jnp.int32)]
        return jnp.concatenate([a] + gap + [b] + gap, axis=1)

    own = jnp.stack([pair(jnp.where(alive, src[...], -1), dst[...]), pair(picked[...], picked[...])])
    near_v[...] = jnp.where(fill, jnp.concatenate([own] * Y, axis=1), 0)
    mine.wait()
    offer = jnp.concatenate([xq[chosen[0, k]] for k in range(NEG)], axis=0)
    pool[z, x, c] = encode(offer).reshape(NEG, R, D)
    pl.semaphore_wait(barrier, XC + Z + Y - 3)
    ids_y = start(y_stage(0, lambda to: near_v, near.at[q]))
    pool_z = start(z_stage(0, lambda to: pool.at[z, x, c], pool.at[z, x, c]))

    G = 16 if NB % 16 == 0 else NB
    n = G * R
    i0 = lax.broadcasted_iota(jnp.int32, (n, n), 0)
    i1 = lax.broadcasted_iota(jnp.int32, (n, n), 1)
    perm = jnp.where(i1 == (i0 & (G - 1)) * R + (i0 >> bits(G)), 1.0, 0.0).astype(jnp.bfloat16)

    def rows(g, _):
        at = pl.multiple_of(g * G, G)
        e = encode(xq[pl.ds(at, G)].reshape(n, D))
        t = jnp.dot(perm, e, preferred_element_type=jnp.float32).astype(jnp.bfloat16)
        for k in range(C):
            send[:, k, pl.ds(at, G), :] = t[:, k * H : (k + 1) * H].reshape(R, G, H)
        return 0

    lax.fori_loop(0, NB // G, rows, 0)

    def bulk(k):
        to = ahead(k)
        return copy(send.at[to // C, to % C], recv.at[me], bulk_s.at[k], bulk_r.at[k], to, q)

    def turn(i):
        return jnp.where(i % 2 == 1, (i + 1) // 2, (Z - i // 2) % Z)

    def column(m):
        return bulk(turn(m // C) * XC + m % C)

    side = (X - 1) * C

    def others(m):
        return bulk(turn(m // side) * XC + C + m % side)

    def column_go(m, _):
        column(m).start()
        return 0

    def others_go(m, _):
        others(m).start()
        return 0

    arrived(ids_y)
    tile = near_v[...]
    for j in range(1, Y):
        tile = tile + near[(q + j) % Y]
    near[q] = tile
    ids[z, xc] = tile[0]
    ids_z = start(z_stage(1, lambda to: ids.at[z, xc], ids.at[z, xc]))
    scalars = pltpu.make_async_copy(near.at[q], near_s, local)
    scalars.start()
    arrived(pool_z)
    pool_x = []
    for dx in range(1, X):
        to = z * XC + ((x + dx) % X) * C + c
        pool_x.append(copy(pool.at[:, x, c], pool.at[:, x, c], c_s.at[0, dx], c_r.at[0, dx], to, q))
    start(pool_x)
    lax.fori_loop(1, Z * C, column_go, 0)
    recv[me] = send[me // C, me % C]

    def full(g, _):
        slot = g % slots
        fetch(g, slot).wait()
        emb[pl.ds(g * per, per)] = encode(stage[slot].reshape(per * BLK, D)).reshape(per, BLK, D)

        @pl.when(g + slots < chunks)
        def _():
            fetch(g + slots, slot).start()

        return 0

    lax.fori_loop(0, chunks // 4, full, 0)
    arrived(ids_z)
    ids_c = start(c_stage(2, lambda to: ids.at[:, xc], ids.at[:, xc]))
    lax.fori_loop(chunks // 4, chunks, full, 0)
    arrived(pool_x)
    pool_c = []
    for dc in range(1, C):
        to = z * XC + x * C + (c + dc) % C
        pool_c.append(
            copy(pool.at[:, :, c], pool.at[:, :, c], c_s.at[1, dc], c_r.at[1, dc], to, q)
        )
    start(pool_c)
    lax.fori_loop(0, Z * side, others_go, 0)
    scalars.wait()
    arrived(pool_c)

    def negatives(e, _):
        for k in range(4 * CAP):
            r, o = e >> bits(N // 4), (e & (N // 4 - 1)) * 4 + k // CAP
            s = near_s[0, r * CAP + k % CAP, o]
            p = near_s[1, r * CAP + k % CAP, o]
            node = p >> bits(NEG)
            cand = pool[
                node >> bits(XC), (node >> bits(C)) & (X - 1), node & (C - 1), p & (NEG - 1)
            ]
            v = lax.dot_general(
                cand,
                emb[jnp.maximum(s, 0)],
                (((1,), (1,)), ((), ())),
                preferred_element_type=jnp.float32,
            )
            total = jnp.sum(softplus(v * scale), axis=0, keepdims=True)
            negp[r, pl.ds(o * CAP + k % CAP, 1), :] = jnp.where(s >= 0, total, 0.0)
        return 0

    lax.fori_loop(0, Y * N // 4, negatives, 0)
    neg_y = start(y_stage(1, lambda to: negp.at[to], negr.at[q]))

    arrived(ids_c)
    lane = lax.broadcasted_iota(jnp.int32, (N, LANES), 1)
    for k in range(RC):
        a = jnp.concatenate(
            [ids[i // XC, i % XC, pl.ds(k, 1), :].astype(jnp.float32) for i in range(N)], axis=0
        )
        t = jnp.swapaxes(jnp.concatenate([a] * (LANES // N), axis=0), 0, 1)[:N]
        idc[pl.ds(k, N, stride=RC), :] = jnp.where(lane < HALF, t, a)

    number = lax.broadcasted_iota(jnp.int32, (N * RC, LANES), 1).astype(jnp.float32)

    def gather(s):
        hots = []
        for k in range(2):
            at = jnp.full((N * RC, LANES), s + k * HALF, jnp.int32)
            col = jnp.take_along_axis(idc[...], at, axis=1)
            hot = [jnp.where(col == number, 1.0, 0.0).astype(jnp.bfloat16)]
            if NB > LANES:
                rest = jnp.where(col == number + LANES, 1.0, 0.0).astype(jnp.bfloat16)
                hot.append(rest[:, : NB - LANES])
            hots.append(jnp.concatenate(hot, axis=1)[:, :NB])
        hot = jnp.concatenate(hots, axis=0)
        got = jnp.dot(hot, recv[s], preferred_element_type=jnp.float32).astype(jnp.bfloat16)
        ends[s] = got.reshape(2, N * RC, H)

    def node_column(m):
        return behind(turn(m // C) * XC + m % C)

    def node_others(m):
        return behind(turn(m // side) * XC + C + m % side)

    def gather_column(m, _):
        for k in range(2):
            column(2 * m + k).wait_recv()
        for k in range(2):
            gather(node_column(2 * m + k))
        return 0

    def gather_others(m, _):
        for k in range(4):
            others(4 * m + k).wait_recv()
        for k in range(4):
            gather(node_others(4 * m + k))
        return 0

    column(1).wait_recv()
    gather(me)
    gather(node_column(1))
    lax.fori_loop(1, Z * C // 2, gather_column, 0)
    lax.fori_loop(0, Z * side // 4, gather_others, 0)

    shape = (N, RC, LANES)
    keep = lax.broadcasted_iota(jnp.int32, shape, 0) == lax.broadcasted_iota(jnp.int32, shape, 2)

    def dots(h, _):
        at = pl.multiple_of(h * 4 * RC, 4 * RC)
        b = ends[:, 1, pl.ds(at, 4 * RC), :].astype(jnp.float32)
        for k in range(4):
            i = 4 * h + k
            a = ends[i, 0].astype(jnp.float32).reshape(N, RC, H)
            sums = jnp.sum(a * b[:, k * RC : (k + 1) * RC], axis=2, keepdims=True)
            part[i // XC, (i % XC) // C, i % C] = jnp.sum(jnp.where(keep, sums, 0.0), axis=0)
        return 0

    lax.fori_loop(0, N // 4, dots, 0)

    to = z * XC + x * C + (c + 1) % C
    swap = copy(part.at[:, :, (c + 1) % C], other, die.at[0], die.at[1], to, q)
    swap.start()
    arrived(neg_y)
    neg = negp[q]
    for j in range(1, Y):
        neg = neg + negr[(q + j) % Y]
    neg_out[...] = neg
    loss = jnp.sum(neg) * (1.0 / BLK)
    count = jnp.sum(jnp.where(alive, 1.0, 0.0)) * BLK
    swap.wait_recv()
    v = part[:, :, c] + other[...]
    half[...] = v
    v = v * scale

    def back(k):
        to = ((z + k // X) % Z) * XC + ((x + k % X) % X) * C + c
        return copy(half.at[to // XC, (to % XC) // C], ret.at[z, x], back_s.at[k], back_r.at[k], to, q)

    def back_go(k, _):
        back(k).start()
        return 0

    def back_got(k, _):
        back(k).wait_recv()
        return 0

    lax.fori_loop(1, R, back_go, 0)
    lit = jnp.concatenate([ids[:, k * C + c][:, None] for k in range(X)], axis=1) >= 0
    lit = lit & (lax.broadcasted_iota(jnp.int32, (Z, X, RC, LANES), 3) < N)
    loss = loss + jnp.sum(jnp.where(lit, softplus(-v), 0.0))
    spot = lax.broadcasted_iota(jnp.int32, tot.shape[1:], 1)
    mine_sum = jnp.where(spot == 0, loss, jnp.where(spot == 1, count, 0.0))
    tot[0] = mine_sum
    ret[z, x] = half[z, x]

    add_c = start(c_stage(3, lambda to: tot.at[0], lc.at[xc]))
    lax.fori_loop(1, R, back_got, 0)
    arrived(add_c)
    total = mine_sum
    for k in range(1, XC):
        total = total + lc[behind(k) % XC]
    tot[1] = total
    add_z = start(z_stage(2, lambda to: tot.at[1], lz.at[z]))
    for k in range(R):
        at = pl.multiple_of((q * R + k) * RC, RC)
        tall[pl.ds(at, RC), :] = ret[k // X, k % X]
    for r in range(Y):
        for k in range(CAP):
            rows_b = tall[pl.ds(r * CAP + k, BLK, stride=RC), :]
            ysend[r, k] = jnp.swapaxes(rows_b, 0, 1)[:N]
    back_y = start(y_stage(2, lambda to: ysend.at[to], yrecv.at[q]))
    arrived(add_z)
    for j in range(1, Z):
        total = total + lz[(z + j) % Z]
    tot[2] = total
    add_y = start(y_stage(3, lambda to: tot.at[2], ly.at[q]))
    arrived(back_y)
    for k in range(CAP):
        v = ysend[q, k]
        for j in range(1, Y):
            v = v + yrecv[(q + j) % Y, k]
        pos_out[pl.ds(k, N, stride=CAP), :] = v
    arrived(add_y)
    for j in range(1, Y):
        total = total + ly[(q + j) % Y]
    loss_out[...] = total

    for copies in (ids_y, ids_z, ids_c, pool_z, pool_x, pool_c, neg_y, back_y, add_c, add_z, add_y):
        sent(copies)
    swap.wait_send()

    def bulk_sent(k, _):
        bulk(k).wait_send()
        return 0

    def back_sent(k, _):
        back(k).wait_send()
        return 0

    lax.fori_loop(1, N, bulk_sent, 0)
    lax.fori_loop(1, R, back_sent, 0)


def step(dims, features, w_in, w_out, pos_src, pos_dst, counts, neg_blocks, neg_pick):
    Z, X, C, Y = dims
    XC, N, R = X * C, Z * X * C, Z * X
    total, D = features.shape
    BLK = R * Y
    NB = total // BLK
    H = D // C
    CAP = pos_dst.shape[3]
    RC = Y * CAP
    NEG = neg_blocks.shape[1]
    bf, f32, i32 = jnp.bfloat16, jnp.float32, jnp.int32
    scale = 1.0 / D**0.5
    src, dst, pick = (t.reshape(N, CAP).T for t in (pos_src, pos_dst, neg_pick))
    per, slots = (8, 4) if NB % 8 == 0 else (NB, 1)
    scratch = [
        pltpu.VMEM((NB, R, D), bf),
        pltpu.VMEM((slots, per, BLK, D), bf),
        pltpu.VMEM((NB, BLK, D), bf),
        pltpu.VMEM((R, C, NB, H), bf),
        pltpu.VMEM((N, NB, H), bf),
        pltpu.VMEM((Z, X, C, NEG, R, D), bf),
        pltpu.VMEM((Y, 2, RC, LANES), i32),
        pltpu.VMEM((Z, XC, RC, LANES), i32),
        pltpu.VMEM((N * RC, LANES), f32),
        pltpu.VMEM((2, RC, LANES), i32),
        pltpu.SMEM((2, RC, LANES), i32),
        pltpu.VMEM((N, 2, N * RC, H), bf),
        pltpu.VMEM((Z, X, C, RC, LANES), f32),
        pltpu.VMEM((Z, X, RC, LANES), f32),
        pltpu.VMEM((Z, X, RC, LANES), f32),
        pltpu.VMEM((Z, X, RC, LANES), f32),
        pltpu.VMEM((BLK * RC, LANES), f32),
        pltpu.VMEM((Y, CAP, N, BLK), f32),
        pltpu.VMEM((Y, CAP, N, BLK), f32),
        pltpu.VMEM((Y, N * CAP, BLK), f32),
        pltpu.VMEM((Y, N * CAP, BLK), f32),
        pltpu.VMEM((3, 8, LANES), f32),
        pltpu.VMEM((XC, 8, LANES), f32),
        pltpu.VMEM((Z, 8, LANES), f32),
        pltpu.VMEM((Y, 8, LANES), f32),
        DMA((N,)),
        DMA((N,)),
        DMA((R,)),
        DMA((R,)),
        DMA((4, Y)),
        DMA((4, Y)),
        DMA((4, XC)),
        DMA((4, XC)),
        DMA((3, Z)),
        DMA((3, Z)),
        DMA((2,)),
        DMA,
        DMA((slots,)),
    ]
    pos, neg, sums = pl.pallas_call(
        functools.partial(kernel, dims, scale),
        in_specs=[pl.BlockSpec(memory_space=pl.ANY), pl.BlockSpec(memory_space=pltpu.SMEM)] + [VMEM] * 6,
        out_specs=[VMEM] * 3,
        out_shape=[
            jax.ShapeDtypeStruct((N * CAP, BLK), f32),
            jax.ShapeDtypeStruct((N * CAP, BLK), f32),
            jax.ShapeDtypeStruct((8, LANES), f32),
        ],
        scratch_shapes=scratch,
        compiler_params=pltpu.CompilerParams(
            collective_id=0, has_side_effects=True, vmem_limit_bytes=60 * 2**20
        ),
        name="step",
    )(features.reshape(NB, BLK, D), neg_blocks, w_in, w_out, src, dst, pick, counts.reshape(1, N))
    loss = sums[0, 0] / sums[0, 1]
    shape = (1, 1, N, CAP, BLK)
    return (pos * scale).reshape(shape), (neg * (1.0 / BLK)).reshape(shape), loss


def solution(mesh):
    n, reps = mesh.shape["node"], mesh.shape["rep"]
    dims = (n // 8, 4, 2, reps) if n >= 32 else (n // 4, 2, 2, reps)
    return jax.shard_map(
        functools.partial(step, dims),
        mesh=mesh,
        in_specs=(
            P("node", None),
            P(),
            P(),
            P("node", "rep", None, None),
            P("node", "rep", None, None),
            P("node", "rep", None),
            P("node", None),
            P("node", "rep", None, None),
        ),
        out_specs=(P("node", "rep", None, None, None), P("node", "rep", None, None, None), P()),
        check_vma=False,
    )
```
